256 devices in a mesh: row: 8 (over y, z_lo), col: 32 (over x, z_hi, core).
Axes of the slice: x: 4, y: 4, z: 8 (z_hi: 4, z_lo: 2; z = z_hi * 2 + z_lo), core: 2. Of those that a mesh axis runs over, the one named last changes fastest.
Arguments:
- queries: bfloat16 [32768, 128], P(('row', 'col')), may hold values from -8 to 8
- key_rows: bfloat16 [32768, 128], P(('row', 'col')), may hold values from -8 to 8
- value_rows: bfloat16 [32768, 128], P(('row', 'col')), may hold values from -6 to 6
- grad_output: bfloat16 [32768, 128], P(('row', 'col')), may hold values from -6 to 6
- positions: int32 [32768], replicated, may hold values from 0 to 32767, as said below
Outputs:
- grad_queries: bfloat16 [32768, 128], P(('row', 'col'))
- grad_keys: bfloat16 [32768, 128], P(('row', 'col'))
- grad_values: bfloat16 [32768, 128], P(('row', 'col'))
The draws below stay inside these ranges and needn't reach their ends.
Inputs may be any that keep to these rules, and one draw needn't show every extreme that they name: `positions`: a permutation: each of 0 to 32767 appears once.
All inputs are finite; a program needn't handle non-finite values.
Results may differ from the reference program's by a relative error of at most 0.0068.
Values may be sent and summed in bfloat16 or wider, within the bound.
A program may use at most 128 MiB of HBM per device.

```python
import math
import jax
import jax.numpy as jnp
from jax import lax

D = 128
TOKENS = 32768


def make_positions(key):
    return jax.random.permutation(jax.random.fold_in(key, 11), TOKENS).astype(jnp.int32)


def draw_positions(key, part):
    return make_positions(key)


def draw_queries(key, part):
    base = jax.random.normal(jax.random.fold_in(key, 21), (TOKENS, D), jnp.float32)
    return jnp.clip(base, -8.0, 8.0).astype(jnp.bfloat16)


def draw_key_rows(key, part):
    base = jax.random.normal(jax.random.fold_in(key, 22), (TOKENS, D), jnp.float32)
    return jnp.clip(base, -8.0, 8.0).astype(jnp.bfloat16)


def block_scale(own_key, shape, cuts, smallest, largest):
    def one(axis_at, blocks):
        steps = jax.random.uniform(jax.random.fold_in(jax.random.fold_in(own_key, 6), axis_at), (blocks,), jnp.float32, smallest / len(cuts), largest / len(cuts))
        return jnp.repeat(jnp.exp(steps), shape[axis_at] // blocks).reshape((-1,) + (1,) * (len(shape) - axis_at - 1))

    gain = one(*cuts[0])
    for cut in cuts[1:]:
        gain = gain * one(*cut)
    return gain


def normal_values(key, extent, width, limit, pieces=(), kind=jnp.bfloat16):
    entries = width * jax.random.normal(key, extent, jnp.float32)
    if pieces:
        entries = entries * block_scale(key, extent, pieces, -0.22, 0.18)
    return jnp.clip(entries, -limit, limit).astype(kind)


def setup_inputs(seed: int = 0) -> dict:
    seeds = jax.random.split(jax.random.key(seed), 6)
    return {
        "queries": draw_queries(jax.random.fold_in(seeds[5], 71), 0),
        "key_rows": draw_key_rows(jax.random.fold_in(seeds[5], 71), 0),
        "value_rows": normal_values(seeds[2], (TOKENS, D), 1.0, 6.0, ((0, 256),)),
        "grad_output": normal_values(seeds[3], (TOKENS, D), 1.0, 6.0, ((0, 256),)),
        "positions": draw_positions(jax.random.fold_in(seeds[5], 71), 0),
    }


def reference(queries, key_rows, value_rows, grad_output, positions):
    score_scale = 1.0 / math.sqrt(D)
    block_rows = 1024 if TOKENS % 1024 == 0 else TOKENS
    blocks_total = TOKENS // block_rows

    def query_block_step(state_pair, which):
        grad_keys, grad_values = state_pair
        begin_row = (which * block_rows).astype(jnp.int32)
        query_block = lax.dynamic_slice_in_dim(queries, begin_row, block_rows, 0)
        grad_block = lax.dynamic_slice_in_dim(grad_output, begin_row, block_rows, 0)
        query_order = lax.dynamic_slice_in_dim(positions, begin_row, block_rows, 0)
        scores = jnp.dot(query_block, key_rows.T, preferred_element_type=jnp.float32) * score_scale
        allowed = query_order[:, None] >= positions[None, :]
        run_max = lax.optimization_barrier(jnp.max(jnp.where(allowed, scores, -1e+30), axis=1, keepdims=True))
        run_sum = lax.optimization_barrier(jnp.sum(jnp.where(allowed, jnp.exp(scores - run_max), 0.0), axis=1, keepdims=True))
        log_total = run_max + jnp.log(run_sum)
        probs = jnp.where(allowed, jnp.exp(scores - log_total), 0.0)
        dprobs = jnp.dot(grad_block, value_rows.T, preferred_element_type=jnp.float32)
        delta = lax.optimization_barrier(jnp.sum(probs * dprobs, axis=1, keepdims=True))
        dscores = (probs * (dprobs - delta)).astype(jnp.bfloat16)
        probs_low = probs.astype(jnp.bfloat16)
        grad_query = jnp.dot(dscores, key_rows, preferred_element_type=jnp.float32) * score_scale
        grad_keys = grad_keys + jnp.dot(dscores.T, query_block, preferred_element_type=jnp.float32) * score_scale
        grad_values = grad_values + jnp.dot(probs_low.T, grad_block, preferred_element_type=jnp.float32)
        return ((grad_keys, grad_values), grad_query)
    zeros_pair = (jnp.zeros((TOKENS, D), jnp.float32), jnp.zeros((TOKENS, D), jnp.float32))
    (grad_keys, grad_values), grad_queries = lax.scan(query_block_step, zeros_pair, jnp.arange(blocks_total, dtype=jnp.int32))
    grad_queries = grad_queries.reshape(TOKENS, D)
    return (grad_queries.astype(jnp.bfloat16), grad_keys.astype(jnp.bfloat16), grad_values.astype(jnp.bfloat16))
```

```python
import math

import jax
import jax.numpy as jnp
from jax import lax
from jax.experimental import pallas as pl
from jax.experimental.pallas import tpu as pltpu
from jax.sharding import PartitionSpec as P

MESH = pl.DeviceIdType.MESH
F32 = jnp.float32
BF16 = jnp.bfloat16
B = 128
NEG = -1e30
FLOOR = -1e6
LOG2E = math.log2(math.e)


def device(x, y, z, c):
    return (y * 2 + lax.rem(z, 2), (x * 4 + lax.div(z, 2)) * 2 + c)


def nt(a, b):
    return lax.dot_general(a, b, (((1,), (1,)), ((), ())), preferred_element_type=F32)


def nn(a, b):
    return jnp.dot(a, b, preferred_element_type=F32)


def kernel(
    q_ref, k_ref, v_ref, g_ref, pos_ref, dq_ref, dk_ref, dv_ref,
    qb, gb, kb, vb, ktb, posk, posq, w_buf, dp_buf, mt, stat_out, stat_in, lse, dlt,
    dqt, part, tmp, pair_out, pair_in, z_out, z_in, q_out, q_in,
    gs, gr, ss, sr, ps, pr, zs, zr, qs_sem, qr_sem,
):
    row, col = lax.axis_index("row"), lax.axis_index("col")
    y, zlo = lax.div(row, 2), lax.rem(row, 2)
    x, c = lax.div(col, 8), lax.rem(col, 2)
    z = lax.rem(lax.div(col, 2), 4) * 2 + zlo
    up4 = lambda a, d: lax.rem(a + d, 4)
    up8 = lambda a, d: lax.rem(a + d, 8)
    other = 1 - c
    mine = x * 4 + y
    chip_scale = LOG2E / math.sqrt(B)

    plane = [lax.rem(mine + d, 16) for d in range(1, 16)]
    plane_dev = [device(lax.div(s, 4), lax.rem(s, 4), z, c) for s in plane]
    barrier = pltpu.get_barrier_semaphore()
    peers = list(plane_dev) + [device(x, y, z, other)]
    peers += [device(x, y, up8(z, d), c) for d in range(1, 8)]
    for p in peers:
        pl.semaphore_signal(barrier, inc=1, device_id=p, device_id_type=MESH)
    pl.semaphore_wait(barrier, len(peers))

    sent = []

    def send(src, dst, send_sem, recv_sem, to):
        copy = pltpu.make_async_remote_copy(
            src_ref=src, dst_ref=dst, send_sem=send_sem, recv_sem=recv_sem, device_id=to, device_id_type=MESH
        )
        copy.start()
        sent.append(copy)
        return copy

    count = [0]

    def gsend(src, dst, to):
        i = count[0]
        count[0] += 1
        return send(src, dst, gs.at[i], gr.at[i], to)

    slot = lambda a, b: a * 4 + b
    xr, xl, yr, yl = up4(x, 1), up4(x, 3), up4(y, 1), up4(y, 3)
    x2, y2 = up4(x, 2), up4(y, 2)
    to_xr, to_xl = device(xr, y, z, c), device(xl, y, z, c)
    to_yr, to_yl = device(x, yr, z, c), device(x, yl, z, c)
    to_zr, to_zl = device(x, y, up8(z, 1), c), device(x, y, up8(z, 7), c)
    to_pair = device(x, y, z, other)
    half0, half1 = pl.ds(0, 64), pl.ds(64, 64)

    plans = []
    for buf, own, first in ((qb, q_ref, True), (gb, g_ref, False)):
        if first:
            at = lambda i, j: slot(i, j)
            a, b, ar, al, br, bl, a2, b2 = x, y, xr, xl, yr, yl, x2, y2
            to_ar, to_al, to_br, to_bl = to_xr, to_xl, to_yr, to_yl
        else:
            at = lambda i, j: slot(j, i)
            a, b, ar, al, br, bl, a2, b2 = y, x, yr, yl, xr, xl, y2, x2
            to_ar, to_al, to_br, to_bl = to_yr, to_yl, to_xr, to_xl
        plans.append((buf, own, at, a, b, ar, al, br, bl, a2, b2, to_ar, to_al, to_br, to_bl))

    zin_r, zin_l = {}, {}
    kv = ((kb, k_ref), (vb, v_ref))
    kslot = lambda zz, cc: zz * 2 + cc
    pair_copies = []
    state = []
    for buf, own, at, a, b, ar, al, br, bl, a2, b2, to_ar, to_al, to_br, to_bl in plans:
        here = buf.at[at(a, b)]
        state.append(
            dict(
                r=gsend(own, here, to_ar),
                l=gsend(own, here, to_al),
                ups=[gsend(own, here, to_br)],
                downs=[gsend(own, here, to_bl)],
            )
        )
    for w, (buf, own) in enumerate(kv):
        here = buf.at[kslot(z, c)]
        zin_r[w, 1] = gsend(own, here, to_zr)
        zin_l[w, 1] = gsend(own, here, to_zl)
        pair_copies.append(gsend(own, here, to_pair))

    qb[mine] = q_ref[...]
    gb[mine] = g_ref[...]
    kb[kslot(z, c)] = k_ref[...]
    vb[kslot(z, c)] = v_ref[...]
    zhi_col = lax.div(z, 2) * 2 + c
    for s in range(16):
        i, j = s // 4, s % 4
        posq[pl.ds(s, 1), :] = pos_ref[pl.ds((j * 2 + zlo) * 32 + i * 8 + zhi_col, 1), :].astype(F32)
    for s in range(16):
        zz, cc = s // 2, s % 2
        line = pos_ref[pl.ds((y * 2 + zz % 2) * 32 + (x * 4 + zz // 2) * 2 + cc, 1), :].astype(F32)
        posk[s] = jnp.broadcast_to(line, (B, B)).T

    def forward_kv(h):
        for w, (buf, _) in enumerate(kv):
            from_l = zin_r.get((w, h))
            from_r = zin_l.get((w, h))
            if from_l is not None:
                from_l.wait_recv()
                src = buf.at[kslot(up8(z, 8 - h), c)]
                if h < 3 or (h == 3 and w == 0):
                    zin_r[w, h + 1] = gsend(src, src, to_zr)
                pair_copies.append(gsend(src, src, to_pair))
            if from_r is not None:
                from_r.wait_recv()
                src = buf.at[kslot(up8(z, h), c)]
                if h < 3 or (h == 3 and w == 1):
                    zin_l[w, h + 1] = gsend(src, src, to_zl)
                pair_copies.append(gsend(src, src, to_pair))

    for st, (buf, own, at, a, b, ar, al, br, bl, a2, b2, to_ar, to_al, to_br, to_bl) in zip(state, plans):
        st["r"].wait_recv()
        src = buf.at[at(al, b)]
        st["r2"] = gsend(src.at[half0], src.at[half0], to_ar)
        st["ups"].append(gsend(src, src, to_br))
        st["downs"].append(gsend(src, src, to_bl))
        st["l"].wait_recv()
        src = buf.at[at(ar, b)]
        st["l2"] = gsend(src.at[half1], src.at[half1], to_al)
        st["ups"].append(gsend(src, src, to_br))
        st["downs"].append(gsend(src, src, to_bl))
    forward_kv(1)
    for st, (buf, own, at, a, b, ar, al, br, bl, a2, b2, to_ar, to_al, to_br, to_bl) in zip(state, plans):
        st["r2"].wait_recv()
        st["l2"].wait_recv()
        src = buf.at[at(a2, b)]
        st["ups"].append(gsend(src, src, to_br))
        st["downs"].append(gsend(src, src, to_bl))
    forward_kv(2)
    last = []
    for st, (buf, own, at, a, b, ar, al, br, bl, a2, b2, to_ar, to_al, to_br, to_bl) in zip(state, plans):
        for n, ia in enumerate((a, al, ar, a2)):
            st["ups"][n].wait_recv()
            src = buf.at[at(ia, bl)]
            last.append(gsend(src.at[half0], src.at[half0], to_br))
            st["downs"][n].wait_recv()
            src = buf.at[at(ia, br)]
            last.append(gsend(src.at[half1], src.at[half1], to_bl))
    forward_kv(3)
    forward_kv(4)
    for copy in last:
        copy.wait_recv()
    for copy in pair_copies:
        copy.wait_recv()

    for zz in range(8):
        ktb[zz] = kb[pl.ds(2 * zz, 2)].reshape(2 * B, B).T

    def scores(t, carry):
        q_tile = qb[pl.ds(4 * t, 4)].reshape(4 * B, B)
        g_tile = gb[pl.ds(4 * t, 4)].reshape(4 * B, B)
        pq = jnp.concatenate([posq[pl.ds(4 * t + j, 1), :] for j in range(4)], axis=1)
        maxes, sums, dots = [], [], []
        for zz in range(8):
            k_tile = kb[2 * zz : 2 * zz + 2].reshape(2 * B, B)
            v_tile = vb[2 * zz : 2 * zz + 2].reshape(2 * B, B)
            s = nt(k_tile, q_tile)
            dp = nt(v_tile, g_tile)
            pk = posk[2 * zz : 2 * zz + 2].reshape(2 * B, B)
            pk = jnp.concatenate([pk] * 4, axis=1)
            s = jnp.where(pq >= pk, s, NEG)
            m = jnp.maximum(jnp.max(s, axis=0, keepdims=True), FLOOR)
            w = jnp.exp2((s - m) * chip_scale)
            w_buf[t, zz] = w
            dp_buf[t, zz] = dp
            mt[t, pl.ds(zz, 1), :] = m * chip_scale
            maxes.append(m)
            sums.append(jnp.sum(w, axis=0, keepdims=True))
            dots.append(jnp.sum(w * dp, axis=0, keepdims=True))
        top = maxes[0]
        for m in maxes[1:]:
            top = jnp.maximum(top, m)
        total = jnp.zeros_like(top)
        dot = jnp.zeros_like(top)
        for m, a, d in zip(maxes, sums, dots):
            f = jnp.exp2((m - top) * chip_scale)
            total += a * f
            dot += d * f
        some = total > 0.0
        safe = jnp.where(some, total, 1.0)
        level = jnp.where(some, top * chip_scale + jnp.log(safe) * LOG2E, NEG)
        mean = dot / safe
        for j in range(4):
            stat_out[t, pl.ds(j, 1), :] = level[:, j * B : (j + 1) * B]
            stat_out[t, pl.ds(4 + j, 1), :] = mean[:, j * B : (j + 1) * B]
        stat_in[t, mine] = stat_out[t]
        for d in range(15):
            pltpu.make_async_remote_copy(
                src_ref=stat_out.at[t], dst_ref=stat_in.at[t, mine], send_sem=ss.at[t, d], recv_sem=sr.at[t, d],
                device_id=plane_dev[d], device_id_type=MESH,
            ).start()
        return carry

    lax.fori_loop(0, 4, scores, 0)

    def combine(t, carry):
        for d in range(15):
            copy = pltpu.make_async_remote_copy(
                src_ref=stat_out.at[t], dst_ref=stat_in.at[t, lax.rem(mine + 15 - d, 16)], send_sem=ss.at[t, d],
                recv_sem=sr.at[t, d], device_id=plane_dev[d], device_id_type=MESH,
            )
            copy.wait_recv()
            copy.wait_send()
        level = stat_in[t, :, 0:4, :]
        mean = stat_in[t, :, 4:8, :]
        top = jnp.max(level, axis=0)
        e = jnp.exp2(level - top[None])
        total = jnp.sum(e, axis=0)
        lse[t] = top + jnp.log(total) * LOG2E
        dlt[t] = jnp.sum(e * mean, axis=0) / total
        return carry

    lax.fori_loop(0, 4, combine, 0)

    def pair_copy(zz):
        return pltpu.make_async_remote_copy(
            src_ref=pair_out.at[zz], dst_ref=pair_in.at[zz], send_sem=ps.at[zz], recv_sem=pr.at[zz],
            device_id=to_pair, device_id_type=MESH,
        )

    def z_copy(zz):
        return pltpu.make_async_remote_copy(
            src_ref=z_out.at[zz], dst_ref=z_in.at[z], send_sem=zs.at[zz], recv_sem=zr.at[z],
            device_id=device(x, y, zz, c), device_id_type=MESH,
        )

    def order(i):
        h = lax.div(i + 1, 2)
        return up8(z, 4 + jnp.where(lax.rem(i, 2) == 1, -h, h))

    def pass_on(zz):
        pair_copy(zz).wait_recv()
        z_out[zz] = (part[zz] + pair_in[zz].astype(F32)).astype(BF16)
        z_copy(zz).start()

    dqt[...] = jnp.zeros_like(dqt)

    def gradients(i, carry):
        zz = order(i)
        k_cols = ktb[zz]
        dk = jnp.zeros((2 * B, B), F32)
        dv = jnp.zeros((2 * B, B), F32)
        for t in range(4):
            level = jnp.concatenate([lse[t, j : j + 1, :] for j in range(4)], axis=1)
            mean = jnp.concatenate([dlt[t, j : j + 1, :] for j in range(4)], axis=1)
            f = jnp.exp2(mt[t, pl.ds(zz, 1), :] - level)
            p = w_buf[t, zz] * f
            ds = (p * (dp_buf[t, zz] - mean)).astype(BF16)
            dv += nn(p.astype(BF16), gb[4 * t : 4 * t + 4].reshape(4 * B, B))
            dk += nn(ds, qb[4 * t : 4 * t + 4].reshape(4 * B, B))
            dqt[t] += nn(k_cols, ds)
        tmp[0] = dk.reshape(2, B, B)
        tmp[1] = dv.reshape(2, B, B)
        part[zz, 0] = tmp[0, c]
        part[zz, 1] = tmp[1, c]
        pair_out[zz, 0] = tmp[0, other].astype(BF16)
        pair_out[zz, 1] = tmp[1, other].astype(BF16)
        pair_copy(zz).start()

        @pl.when(i > 0)
        def _():
            pass_on(order(i - 1))

        return carry

    lax.fori_loop(0, 8, gradients, 0)

    def q_copy(d):
        s = plane[d]
        return pltpu.make_async_remote_copy(
            src_ref=q_out.at[s], dst_ref=q_in.at[mine], send_sem=qs_sem.at[d], recv_sem=qr_sem.at[d],
            device_id=plane_dev[d], device_id_type=MESH,
        )

    for s in range(16):
        q_out[s] = dqt[s // 4, :, (s % 4) * B : (s % 4 + 1) * B].astype(BF16)
    for d in range(15):
        q_copy(d).start()

    scale = 1.0 / math.sqrt(B)
    pair_copy(z).wait_recv()
    acc = part[z] + pair_in[z].astype(F32)
    for d in range(1, 8):
        src = up8(z, 8 - d)
        pltpu.make_async_remote_copy(
            src_ref=z_out.at[src], dst_ref=z_in.at[src], send_sem=zs.at[src], recv_sem=zr.at[src],
            device_id=device(x, y, src, c), device_id_type=MESH,
        ).wait_recv()
        acc += z_in[src].astype(F32)
    dk_ref[...] = (acc[0] * scale).astype(BF16)
    dv_ref[...] = acc[1].astype(BF16)

    own = q_out[mine].astype(F32)
    for d in range(15):
        q_copy(d).wait_recv()
        own += q_in[lax.rem(mine + 15 - d, 16)].astype(F32)
    dq_ref[...] = (own * scale).T.astype(BF16)

    for copy in sent:
        copy.wait_send()
    for zz in range(8):
        pair_copy(zz).wait_send()
    for d in range(1, 8):
        z_copy(up8(z, d)).wait_send()
    for d in range(15):
        q_copy(d).wait_send()


def body(queries, key_rows, value_rows, grad_output, positions):
    vmem = pl.BlockSpec(memory_space=pltpu.VMEM)
    out = jax.ShapeDtypeStruct((B, B), BF16)
    dma = pltpu.SemaphoreType.DMA
    blocks = pltpu.VMEM((16, B, B), BF16)
    return pl.pallas_call(
        kernel,
        out_shape=(out, out, out),
        in_specs=[vmem] * 5,
        out_specs=(vmem,) * 3,
        scratch_shapes=[
            blocks, blocks, blocks, blocks,
            pltpu.VMEM((8, B, 2 * B), BF16),
            pltpu.VMEM((16, B, B), F32),
            pltpu.VMEM((16, B), F32),
            pltpu.VMEM((4, 8, 2 * B, 4 * B), F32),
            pltpu.VMEM((4, 8, 2 * B, 4 * B), F32),
            pltpu.VMEM((4, 8, 4 * B), F32),
            pltpu.VMEM((4, 8, B), F32),
            pltpu.VMEM((4, 16, 8, B), F32),
            pltpu.VMEM((4, 4, B), F32),
            pltpu.VMEM((4, 4, B), F32),
            pltpu.VMEM((4, B, 4 * B), F32),
            pltpu.VMEM((8, 2, B, B), F32),
            pltpu.VMEM((2, 2, B, B), F32),
            pltpu.VMEM((8, 2, B, B), BF16),
            pltpu.VMEM((8, 2, B, B), BF16),
            pltpu.VMEM((8, 2, B, B), BF16),
            pltpu.VMEM((8, 2, B, B), BF16),
            pltpu.VMEM((16, B, B), BF16),
            pltpu.VMEM((16, B, B), BF16),
            dma((70,)), dma((70,)),
            dma((4, 15)), dma((4, 15)),
            dma((8,)), dma((8,)),
            dma((8,)), dma((8,)),
            dma((15,)), dma((15,)),
        ],
        compiler_params=pltpu.CompilerParams(
            collective_id=0, has_side_effects=True, vmem_limit_bytes=60 * 1024 * 1024
        ),
        name="attention_backward",
    )(queries, key_rows, value_rows, grad_output, positions.reshape(-1, B))


def solution(mesh):
    spec = P(("row", "col"), None)
    return jax.shard_map(
        body,
        mesh=mesh,
        in_specs=(spec, spec, spec, spec, P()),
        out_specs=(spec, spec, spec),
        check_vma=False,
    )
```

```python
import math

import jax
import jax.numpy as jnp
from jax import lax
from jax.experimental import pallas as pl
from jax.experimental.pallas import tpu as pltpu
from jax.sharding import PartitionSpec as P

MESH = pl.DeviceIdType.MESH
F32 = jnp.float32
BF16 = jnp.bfloat16
B = 128
NEG = -1e30
FLOOR = -1e6
LOG2E = math.log2(math.e)


def device(x, y, z, c):
    return (y * 2 + lax.rem(z, 2), (x * 4 + lax.div(z, 2)) * 2 + c)


def nt(a, b):
    return lax.dot_general(a, b, (((1,), (1,)), ((), ())), preferred_element_type=F32)


def nn(a, b):
    return jnp.dot(a, b, preferred_element_type=F32)


def kernel(
    q_ref, k_ref, v_ref, g_ref, pos_hbm, out_ref,
    qb, gb, kb, vb, pos_ref, ktb, posk, posq, s_buf, dp_buf, mt, zt, dt, stat_out, stat_in, lse, dlt,
    dqt, part, tmp, pair_out, pair_in, z_out, z_in, q_out, q_in,
    ins, gs, gr, ss, sr, ps, pr, zs, zr, qs_sem, qr_sem,
):
    row, col = lax.axis_index("row"), lax.axis_index("col")
    y, zlo = lax.div(row, 2), lax.rem(row, 2)
    x, c = lax.div(col, 8), lax.rem(col, 2)
    z = lax.rem(lax.div(col, 2), 4) * 2 + zlo
    up4 = lambda a, d: lax.rem(a + d, 4)
    up8 = lambda a, d: lax.rem(a + d, 8)
    other = 1 - c
    mine = x * 4 + y
    chip_scale = LOG2E / math.sqrt(B)

    here_k = z * 2 + c
    fetch = [
        pltpu.make_async_copy(src, dst, ins.at[n])
        for n, (src, dst) in enumerate(
            ((k_ref, kb.at[here_k]), (v_ref, vb.at[here_k]), (q_ref, qb.at[mine]), (g_ref, gb.at[mine]), (pos_hbm, pos_ref))
        )
    ]
    for copy in fetch:
        copy.start()

    plane = [lax.rem(mine + d, 16) for d in range(1, 16)]
    plane_dev = [device(lax.div(s, 4), lax.rem(s, 4), z, c) for s in plane]
    barrier = pltpu.get_barrier_semaphore()
    peers = [device(up4(x, d), y, z, c) for d in (1, 3)] + [device(x, up4(y, d), z, c) for d in (1, 3)]
    peers += [device(x, y, up8(z, d), c) for d in (1, 7)] + [device(x, y, z, other)]
    for p in peers:
        pl.semaphore_signal(barrier, inc=1, device_id=p, device_id_type=MESH)
    for copy in fetch[:4]:
        copy.wait()
    pl.semaphore_wait(barrier, len(peers))

    sent = []

    def send(src, dst, send_sem, recv_sem, to):
        copy = pltpu.make_async_remote_copy(
            src_ref=src, dst_ref=dst, send_sem=send_sem, recv_sem=recv_sem, device_id=to, device_id_type=MESH
        )
        copy.start()
        sent.append(copy)
        return copy

    count = [0]

    def gsend(src, dst, to):
        i = count[0]
        count[0] += 1
        return send(src, dst, gs.at[i], gr.at[i], to)

    slot = lambda a, b: a * 4 + b
    xr, xl, yr, yl = up4(x, 1), up4(x, 3), up4(y, 1), up4(y, 3)
    x2, y2 = up4(x, 2), up4(y, 2)
    to_xr, to_xl = device(xr, y, z, c), device(xl, y, z, c)
    to_yr, to_yl = device(x, yr, z, c), device(x, yl, z, c)
    to_zr, to_zl = device(x, y, up8(z, 1), c), device(x, y, up8(z, 7), c)
    to_pair = device(x, y, z, other)
    half0, half1 = pl.ds(0, 64), pl.ds(64, 64)

    done = set()

    def need(*copies):
        for copy in copies:
            if id(copy) not in done:
                done.add(id(copy))
                copy.wait_recv()

    plans = []
    for buf, first in ((qb, True), (gb, False)):
        if first:
            at = lambda i, j: slot(i, j)
            a, b, ar, al, br, bl, a2 = x, y, xr, xl, yr, yl, x2
            to_ar, to_al, to_br, to_bl = to_xr, to_xl, to_yr, to_yl
        else:
            at = lambda i, j: slot(j, i)
            a, b, ar, al, br, bl, a2 = y, x, yr, yl, xr, xl, y2
            to_ar, to_al, to_br, to_bl = to_yr, to_yl, to_xr, to_xl
        plans.append((dict(), buf, at, a, b, ar, al, br, bl, a2, to_ar, to_al, to_br, to_bl))

    zin_r, zin_l, pair = {}, {}, {}
    kv = (kb, vb)
    kslot = lambda zz, cc: zz * 2 + cc

    def forward_kv(h):
        for w, buf in enumerate(kv):
            for came, far, to_next, off in ((zin_r, 0, to_zr, 8 - h), (zin_l, 1, to_zl, h)):
                if h and (w, h) not in came:
                    continue
                if h:
                    need(came[w, h])
                src = buf.at[kslot(up8(z, off % 8), c)]
                if h < 3 or (h == 3 and w == far):
                    came[w, h + 1] = gsend(src, src, to_next)
                if h or not far:
                    pair[w, off % 8] = gsend(src, src, to_pair)

    def across(st, buf, at, ia, b, to_br, to_bl, n):
        src = buf.at[at(ia, b)]
        st["up", n] = gsend(src, src, to_br)
        st["down", n] = gsend(src, src, to_bl)

    def across_last(st, buf, at, ia, br, bl, to_br, to_bl, n):
        need(st["up", n])
        src = buf.at[at(ia, bl)].at[half0]
        st["lu", n] = gsend(src, src, to_br)
        need(st["down", n])
        src = buf.at[at(ia, br)].at[half1]
        st["ld", n] = gsend(src, src, to_bl)

    forward_kv(0)
    for st, buf, at, a, b, ar, al, br, bl, a2, to_ar, to_al, to_br, to_bl in plans:
        src = buf.at[at(a, b)]
        st["r"] = gsend(src, src, to_ar)
        st["l"] = gsend(src, src, to_al)
        across(st, buf, at, a, b, to_br, to_bl, 0)

    fetch[4].wait()
    zhi_col = lax.div(z, 2) * 2 + c
    for s in range(16):
        i, j = s // 4, s % 4
        posq[pl.ds(s, 1), :] = pos_ref[pl.ds((j * 2 + zlo) * 32 + i * 8 + zhi_col, 1), :].astype(F32)
    for s in range(16):
        zz, cc = s // 2, s % 2
        line = pos_ref[pl.ds((y * 2 + zz % 2) * 32 + (x * 4 + zz // 2) * 2 + cc, 1), :].astype(F32)
        posk[s] = jnp.broadcast_to(line, (B, B)).T

    def tile(t, zz):
        q_tile = qb[pl.ds(4 * t, 4)].reshape(4 * B, B)
        g_tile = gb[pl.ds(4 * t, 4)].reshape(4 * B, B)
        k_tile = kb[pl.ds(2 * zz, 2)].reshape(2 * B, B)
        v_tile = vb[pl.ds(2 * zz, 2)].reshape(2 * B, B)
        pq = jnp.concatenate([posq[pl.ds(4 * t + j, 1), :] for j in range(4)], axis=1)
        pk = posk[pl.ds(2 * zz, 2)].reshape(2 * B, B)
        pk = jnp.concatenate([pk] * 4, axis=1)
        s = jnp.where(pq >= pk, nt(k_tile, q_tile), NEG)
        s_buf[t, zz] = s
        m = jnp.maximum(jnp.max(s, axis=0, keepdims=True), FLOOR)
        dp = nt(v_tile, g_tile)
        dp_buf[t, zz] = dp
        w = jnp.exp2((s - m) * chip_scale)
        mt[t, pl.ds(zz, 1), :] = m
        zt[t, pl.ds(zz, 1), :] = jnp.sum(w, axis=0, keepdims=True)
        dt[t, pl.ds(zz, 1), :] = jnp.sum(w * dp, axis=0, keepdims=True)

    def tiles(n, pick):
        def step(i, carry):
            for t, zz in pick(i):
                tile(t, zz)
            return carry

        lax.fori_loop(0, n, step, 0)

    near = lambda i: up8(z, i + 5 * lax.div(i, 2))
    both = lambda i, d: up8(z, d + i * (8 - 2 * d))

    forward_kv(1)
    for st, buf, at, a, b, ar, al, br, bl, a2, to_ar, to_al, to_br, to_bl in plans:
        need(st["r"])
        src = buf.at[at(al, b)].at[half0]
        st["r2"] = gsend(src, src, to_ar)
        across(st, buf, at, al, b, to_br, to_bl, 1)
        need(st["l"])
        src = buf.at[at(ar, b)].at[half1]
        st["l2"] = gsend(src, src, to_al)
        across(st, buf, at, ar, b, to_br, to_bl, 2)
        across_last(st, buf, at, a, br, bl, to_br, to_bl, 0)
    forward_kv(2)
    for st, buf, at, a, b, ar, al, br, bl, a2, to_ar, to_al, to_br, to_bl in plans:
        need(st["r2"], st["l2"])
        across(st, buf, at, a2, b, to_br, to_bl, 3)
        across_last(st, buf, at, al, br, bl, to_br, to_bl, 1)
        across_last(st, buf, at, ar, br, bl, to_br, to_bl, 2)
    sq, sg = plans[0][0], plans[1][0]
    need(sq["lu", 0], sq["ld", 0], *(pair[w, off] for w in range(2) for off in (0, 1, 7)))
    tiles(3, lambda i: [(x, near(i))])
    for st, buf, at, a, b, ar, al, br, bl, a2, to_ar, to_al, to_br, to_bl in plans:
        across_last(st, buf, at, a2, br, bl, to_br, to_bl, 3)
    need(*(sq[k, n] for k in ("lu", "ld") for n in (1, 2)))
    tiles(3, lambda i: [(xr, near(i)), (xl, near(i))])
    forward_kv(3)
    need(*(pair[w, off] for w in range(2) for off in (2, 6)))
    tiles(2, lambda i: [(x, both(i, 2)), (xr, both(i, 2)), (xl, both(i, 2))])
    need(*(sq[k, 3] for k in ("lu", "ld")), *(sg[k, n] for k in ("lu", "ld") for n in range(4)))
    tiles(3, lambda i: [(x2, near(i))])
    forward_kv(4)
    tiles(2, lambda i: [(x2, both(i, 2))])
    need(*(pair[w, off] for w in range(2) for off in (3, 5)))
    tiles(4, lambda i: [(i, both(0, 3)), (i, both(1, 3))])
    need(*(pair[w, 4] for w in range(2)))

    def finish(t, carry):
        tile(t, up8(z, 4))
        maxes = mt[t]
        top = jnp.max(maxes, axis=0, keepdims=True)
        f = jnp.exp2((maxes - top) * chip_scale)
        total = jnp.sum(zt[t] * f, axis=0, keepdims=True)
        dot = jnp.sum(dt[t] * f, axis=0, keepdims=True)
        some = total > 0.0
        safe = jnp.where(some, total, 1.0)
        level = jnp.where(some, top * chip_scale + jnp.log(safe) * LOG2E, NEG)
        mean = dot / safe
        for j in range(4):
            stat_out[t, pl.ds(j, 1), :] = level[:, j * B : (j + 1) * B]
            stat_out[t, pl.ds(4 + j, 1), :] = mean[:, j * B : (j + 1) * B]
        stat_in[t, mine] = stat_out[t]
        for d in range(15):
            pltpu.make_async_remote_copy(
                src_ref=stat_out.at[t], dst_ref=stat_in.at[t, mine], send_sem=ss.at[t, d], recv_sem=sr.at[t, d],
                device_id=plane_dev[d], device_id_type=MESH,
            ).start()
        return carry

    lax.fori_loop(0, 4, finish, 0)

    for zz in range(8):
        ktb[zz] = kb[pl.ds(2 * zz, 2)].reshape(2 * B, B).T
    dqt[...] = jnp.zeros_like(dqt)

    def combine(t, carry):
        for d in range(15):
            copy = pltpu.make_async_remote_copy(
                src_ref=stat_out.at[t], dst_ref=stat_in.at[t, lax.rem(mine + 15 - d, 16)], send_sem=ss.at[t, d],
                recv_sem=sr.at[t, d], device_id=plane_dev[d], device_id_type=MESH,
            )
            copy.wait_recv()
            copy.wait_send()
        level = stat_in[t, :, 0:4, :]
        mean = stat_in[t, :, 4:8, :]
        top = jnp.max(level, axis=0)
        e = jnp.exp2(level - top[None])
        total = jnp.sum(e, axis=0)
        lse[t] = top + jnp.log(total) * LOG2E
        dlt[t] = jnp.sum(e * mean, axis=0) / total
        return carry

    lax.fori_loop(0, 4, combine, 0)

    def pair_copy(zz):
        return pltpu.make_async_remote_copy(
            src_ref=pair_out.at[zz], dst_ref=pair_in.at[zz], send_sem=ps.at[zz], recv_sem=pr.at[zz],
            device_id=to_pair, device_id_type=MESH,
        )

    def z_copy(zz):
        return pltpu.make_async_remote_copy(
            src_ref=z_out.at[zz], dst_ref=z_in.at[z], send_sem=zs.at[zz], recv_sem=zr.at[z],
            device_id=device(x, y, zz, c), device_id_type=MESH,
        )

    def order(i):
        h = lax.div(i + 1, 2)
        return up8(z, 4 + jnp.where(lax.rem(i, 2) == 1, -h, h))

    def pass_on(zz):
        pair_copy(zz).wait_recv()
        z_out[zz] = (part[zz] + pair_in[zz].astype(F32)).astype(BF16)
        z_copy(zz).start()

    def gradients(i, carry):
        zz = order(i)
        k_cols = ktb[zz]
        dk = jnp.zeros((2 * B, B), F32)
        dv = jnp.zeros((2 * B, B), F32)
        for t in range(4):
            level = jnp.concatenate([lse[t, j : j + 1, :] for j in range(4)], axis=1)
            mean = jnp.concatenate([dlt[t, j : j + 1, :] for j in range(4)], axis=1)
            p = jnp.exp2(s_buf[t, zz] * chip_scale - level)
            ds = (p * (dp_buf[t, zz] - mean)).astype(BF16)
            dv += nn(p.astype(BF16), gb[4 * t : 4 * t + 4].reshape(4 * B, B))
            dk += nn(ds, qb[4 * t : 4 * t + 4].reshape(4 * B, B))
            dqt[t] += nn(k_cols, ds)
        tmp[0] = dk.reshape(2, B, B)
        tmp[1] = dv.reshape(2, B, B)
        part[zz, 0] = tmp[0, c]
        part[zz, 1] = tmp[1, c]
        pair_out[zz, 0] = tmp[0, other].astype(BF16)
        pair_out[zz, 1] = tmp[1, other].astype(BF16)
        pair_copy(zz).start()

        @pl.when(i > 0)
        def _():
            pass_on(order(i - 1))

        return carry

    lax.fori_loop(0, 8, gradients, 0)

    def q_copy(d):
        s = plane[d]
        return pltpu.make_async_remote_copy(
            src_ref=q_out.at[s], dst_ref=q_in.at[mine], send_sem=qs_sem.at[d], recv_sem=qr_sem.at[d],
            device_id=plane_dev[d], device_id_type=MESH,
        )

    for s in range(16):
        q_out[s] = dqt[s // 4, :, (s % 4) * B : (s % 4 + 1) * B].astype(BF16)
    for d in range(15):
        q_copy(d).start()

    scale = 1.0 / math.sqrt(B)
    pair_copy(z).wait_recv()
    acc = part[z] + pair_in[z].astype(F32)
    for d in range(1, 8):
        src = up8(z, 8 - d)
        pltpu.make_async_remote_copy(
            src_ref=z_out.at[src], dst_ref=z_in.at[src], send_sem=zs.at[src], recv_sem=zr.at[src],
            device_id=device(x, y, src, c), device_id_type=MESH,
        ).wait_recv()
        acc += z_in[src].astype(F32)
    out_ref[1] = (acc[0] * scale).astype(BF16)
    out_ref[2] = acc[1].astype(BF16)

    own = q_out[mine].astype(F32)
    for d in range(15):
        q_copy(d).wait_recv()
        own += q_in[lax.rem(mine + 15 - d, 16)].astype(F32)
    out_ref[0] = (own * scale).T.astype(BF16)

    for copy in sent:
        copy.wait_send()
    for zz in range(8):
        pair_copy(zz).wait_send()
    for d in range(1, 8):
        z_copy(up8(z, d)).wait_send()
    for d in range(15):
        q_copy(d).wait_send()


def body(queries, key_rows, value_rows, grad_output, positions):
    vmem = pl.BlockSpec(memory_space=pltpu.VMEM)
    hbm = pl.BlockSpec(memory_space=pl.ANY)
    dma = pltpu.SemaphoreType.DMA
    blocks = pltpu.VMEM((16, B, B), BF16)
    grads = pl.pallas_call(
        kernel,
        out_shape=jax.ShapeDtypeStruct((3, B, B), BF16),
        in_specs=[hbm] * 5,
        out_specs=vmem,
        scratch_shapes=[
            blocks, blocks, blocks, blocks,
            pltpu.VMEM((256, B), jnp.int32),
            pltpu.VMEM((8, B, 2 * B), BF16),
            pltpu.VMEM((16, B, B), F32),
            pltpu.VMEM((16, B), F32),
            pltpu.VMEM((4, 8, 2 * B, 4 * B), F32),
            pltpu.VMEM((4, 8, 2 * B, 4 * B), F32),
            pltpu.VMEM((4, 8, 4 * B), F32),
            pltpu.VMEM((4, 8, 4 * B), F32),
            pltpu.VMEM((4, 8, 4 * B), F32),
            pltpu.VMEM((4, 8, B), F32),
            pltpu.VMEM((4, 16, 8, B), F32),
            pltpu.VMEM((4, 4, B), F32),
            pltpu.VMEM((4, 4, B), F32),
            pltpu.VMEM((4, B, 4 * B), F32),
            pltpu.VMEM((8, 2, B, B), F32),
            pltpu.VMEM((2, 2, B, B), F32),
            pltpu.VMEM((8, 2, B, B), BF16),
            pltpu.VMEM((8, 2, B, B), BF16),
            pltpu.VMEM((8, 2, B, B), BF16),
            pltpu.VMEM((8, 2, B, B), BF16),
            pltpu.VMEM((16, B, B), BF16),
            pltpu.VMEM((16, B, B), BF16),
            dma((5,)),
            dma((70,)), dma((70,)),
            dma((4, 15)), dma((4, 15)),
            dma((8,)), dma((8,)),
            dma((8,)), dma((8,)),
            dma((15,)), dma((15,)),
        ],
        compiler_params=pltpu.CompilerParams(
            collective_id=0, has_side_effects=True, vmem_limit_bytes=60 * 1024 * 1024
        ),
        name="attention_backward",
    )(queries, key_rows, value_rows, grad_output, positions.reshape(-1, B))
    return grads[0], grads[1], grads[2]


def solution(mesh):
    spec = P(("row", "col"), None)
    return jax.shard_map(
        body,
        mesh=mesh,
        in_specs=(spec, spec, spec, spec, P()),
        out_specs=(spec, spec, spec),
        check_vma=False,
    )
```

```python
import math

import jax
import jax.numpy as jnp
from jax import lax
from jax.experimental import pallas as pl
from jax.experimental.pallas import tpu as pltpu
from jax.sharding import PartitionSpec as P

MESH = pl.DeviceIdType.MESH
F32 = jnp.float32
BF16 = jnp.bfloat16
B = 128
NEG = -1e30
FLOOR = -1e6
LOG2E = math.log2(math.e)


def device(x, y, z, c):
    return (y * 2 + lax.rem(z, 2), (x * 4 + lax.div(z, 2)) * 2 + c)


def nt(a, b):
    return lax.dot_general(a, b, (((1,), (1,)), ((), ())), preferred_element_type=F32)


def nn(a, b):
    return jnp.dot(a, b, preferred_element_type=F32)


def kernel(
    q_ref, k_ref, v_ref, g_ref, pos_hbm, out_ref,
    qb, gb, kb, vb, pos_ref, ktb, posk, posq, s_buf, dp_buf, mt, zt, dt, stat_out, stat_in, factor, tops,
    w_buf, e_buf, q_scaled, g_scaled, part, tmp, pair_out, pair_in, z_out, z_in, q_out, q_in,
    ins, gs, gr, ss, sr, ps, pr, zs, zr, qs_sem, qr_sem,
):
    row, col = lax.axis_index("row"), lax.axis_index("col")
    y, zlo = lax.div(row, 2), lax.rem(row, 2)
    x, c = lax.div(col, 8), lax.rem(col, 2)
    z = lax.rem(lax.div(col, 2), 4) * 2 + zlo
    up4 = lambda a, d: lax.rem(a + d, 4)
    up8 = lambda a, d: lax.rem(a + d, 8)
    other = 1 - c
    mine = x * 4 + y
    chip_scale = LOG2E / math.sqrt(B)

    here_k = z * 2 + c
    fetch = [
        pltpu.make_async_copy(src, dst, ins.at[n])
        for n, (src, dst) in enumerate(
            ((k_ref, kb.at[here_k]), (v_ref, vb.at[here_k]), (q_ref, qb.at[mine]), (g_ref, gb.at[mine]), (pos_hbm, pos_ref))
        )
    ]
    for copy in fetch:
        copy.start()

    plane = [lax.rem(mine + d, 16) for d in range(1, 16)]
    plane_dev = [device(lax.div(s, 4), lax.rem(s, 4), z, c) for s in plane]
    barrier = pltpu.get_barrier_semaphore()
    peers = [device(up4(x, d), y, z, c) for d in (2, 1, 3)] + [device(x, up4(y, d), z, c) for d in (2, 1, 3)]
    peers += [device(x, y, up8(z, d), c) for d in (2, 6, 1, 7)] + [device(x, y, z, other)]
    for p in peers:
        pl.semaphore_signal(barrier, inc=1, device_id=p, device_id_type=MESH)
    for copy in fetch[:4]:
        copy.wait()
    pl.semaphore_wait(barrier, len(peers))

    sent = []

    def send(src, dst, send_sem, recv_sem, to):
        copy = pltpu.make_async_remote_copy(
            src_ref=src, dst_ref=dst, send_sem=send_sem, recv_sem=recv_sem, device_id=to, device_id_type=MESH
        )
        copy.start()
        sent.append(copy)
        return copy

    count = [0]

    def gsend(src, dst, to):
        i = count[0]
        count[0] += 1
        return send(src, dst, gs.at[i], gr.at[i], to)

    slot = lambda a, b: a * 4 + b
    xr, xl, yr, yl = up4(x, 1), up4(x, 3), up4(y, 1), up4(y, 3)
    x2, y2 = up4(x, 2), up4(y, 2)
    to_xr, to_xl = device(xr, y, z, c), device(xl, y, z, c)
    to_yr, to_yl = device(x, yr, z, c), device(x, yl, z, c)
    to_pair = device(x, y, z, other)

    done = set()

    def need(*copies):
        for copy in copies:
            if id(copy) not in done:
                done.add(id(copy))
                copy.wait_recv()

    to_x2, to_y2 = device(x2, y, z, c), device(x, y2, z, c)
    plans = (
        ({}, qb, lambda i, j: slot(i, j), x, y, (xl, xr, x2), (to_xr, to_xl, to_x2), (to_yr, to_yl, to_y2)),
        ({}, gb, lambda i, j: slot(j, i), y, x, (yl, yr, y2), (to_yr, to_yl, to_y2), (to_xr, to_xl, to_x2)),
    )
    kv = (kb, vb)
    kslot = lambda zz, cc: zz * 2 + cc
    along, pair = {}, {}

    def send_z(w, off, *steps):
        src = kv[w].at[kslot(up8(z, off), c)]
        for d in steps:
            along[w, (off - d) % 8] = gsend(src, src, device(x, y, up8(z, d), c))

    def send_pair(off):
        for w in range(2):
            if off:
                need(along[w, off])
            src = kv[w].at[kslot(up8(z, off), c)]
            pair[w, off] = gsend(src, src, to_pair)

    for w in range(2):
        send_z(w, 0, 2, 6)
    for st, buf, at, a, b, ias, to_a, to_b in plans:
        src = buf.at[at(a, b)]
        for n in (2, 0, 1):
            st["a", n] = gsend(src, src, to_a[n])
        for n in (2, 0, 1):
            st["b", 3, n] = gsend(src, src, to_b[n])
    for w in range(2):
        send_z(w, 0, 1, 7)
    send_pair(0)

    fetch[4].wait()
    zhi_col = lax.div(z, 2) * 2 + c
    for s in range(16):
        i, j = s // 4, s % 4
        posq[pl.ds(s, 1), :] = pos_ref[pl.ds((j * 2 + zlo) * 32 + i * 8 + zhi_col, 1), :].astype(F32)
    for s in range(16):
        zz, cc = s // 2, s % 2
        line = pos_ref[pl.ds((y * 2 + zz % 2) * 32 + (x * 4 + zz // 2) * 2 + cc, 1), :].astype(F32)
        posk[s] = jnp.broadcast_to(line, (B, B)).T

    def tile(t, zz):
        q_tile = qb[pl.ds(4 * t, 4)].reshape(4 * B, B)
        g_tile = gb[pl.ds(4 * t, 4)].reshape(4 * B, B)
        k_tile = kb[pl.ds(2 * zz, 2)].reshape(2 * B, B)
        v_tile = vb[pl.ds(2 * zz, 2)].reshape(2 * B, B)
        pq = jnp.concatenate([posq[pl.ds(4 * t + j, 1), :] for j in range(4)], axis=1)
        pk = posk[pl.ds(2 * zz, 2)].reshape(2 * B, B)
        pk = jnp.concatenate([pk] * 4, axis=1)
        s = jnp.where(pq >= pk, nt(k_tile, q_tile) * chip_scale, NEG)
        s_buf[t, zz] = s
        m = jnp.maximum(jnp.max(s, axis=0, keepdims=True), FLOOR)
        dp = nt(v_tile, g_tile)
        dp_buf[t, zz] = dp
        w = jnp.exp2(s - m)
        mt[t, pl.ds(zz, 1), :] = m
        zt[t, pl.ds(zz, 1), :] = jnp.sum(w, axis=0, keepdims=True)
        dt[t, pl.ds(zz, 1), :] = jnp.sum(w * dp, axis=0, keepdims=True)

    def tiles(n, pick):
        def step(i, carry):
            for t, zz in pick(i):
                tile(t, zz)
            return carry

        lax.fori_loop(0, n, step, 0)

    near = lambda i: up8(z, i + 5 * lax.div(i, 2))
    both = lambda i, d: up8(z, d + i * (8 - 2 * d))

    for n in range(2):
        for st, buf, at, a, b, ias, to_a, to_b in plans:
            need(st["a", n])
            src = buf.at[at(ias[n], b)]
            for m in (2, 0, 1):
                st["b", n, m] = gsend(src, src, to_b[m])
    for w in range(2):
        need(along[w, 6])
        send_z(w, 6, *((2, 1) if w == 0 else (1,)))
        need(along[w, 2])
        send_z(w, 2, *((6, 7) if w == 1 else (7,)))
    for st, buf, at, a, b, ias, to_a, to_b in plans:
        need(st["a", 2])
        src = buf.at[at(ias[2], b)]
        for m in (2, 0, 1):
            st["b", 2, m] = gsend(src, src, to_b[m])
    for off in (1, 7, 2, 6):
        send_pair(off)
    sq, sg = plans[0][0], plans[1][0]

    def need_column(n):
        need(*(sq["b", n, m] for m in range(3)))
        if n < 3:
            need(*(sg["b", m, n] for m in range(4)))

    need_column(3)
    need(*(pair[w, off] for w in range(2) for off in (0, 1, 7)))
    tiles(3, lambda i: [(x, near(i))])
    need(*(pair[w, off] for w in range(2) for off in (2, 6)))
    tiles(1, lambda i: [(x, both(0, 2)), (x, both(1, 2))])
    need_column(0)
    need_column(1)
    tiles(3, lambda i: [(xl, near(i)), (xr, near(i))])
    for off in (3, 5, 4):
        send_pair(off)
    tiles(2, lambda i: [(xl, both(i, 2)), (xr, both(i, 2))])
    need_column(2)
    tiles(3, lambda i: [(x2, near(i))])
    tiles(1, lambda i: [(x2, both(0, 2)), (x2, both(1, 2))])
    need(*(pair[w, off] for w in range(2) for off in (3, 5)))
    tiles(4, lambda i: [(i, both(0, 3)), (i, both(1, 3))])
    need(*(pair[w, 4] for w in range(2)))

    def finish(t, carry):
        tile(t, up8(z, 4))
        maxes = mt[t]
        top = jnp.max(maxes, axis=0, keepdims=True)
        tops[t, 0:1, :] = top
        f = jnp.exp2(maxes - top)
        total = jnp.sum(zt[t] * f, axis=0, keepdims=True)
        dot = jnp.sum(dt[t] * f, axis=0, keepdims=True)
        some = total > 0.0
        safe = jnp.where(some, total, 1.0)
        level = jnp.where(some, top + jnp.log(safe) * LOG2E, NEG)
        mean = dot / safe
        tops[t, 1:2, :] = mean
        for j in range(4):
            stat_out[t, pl.ds(j, 1), :] = level[:, j * B : (j + 1) * B]
            stat_out[t, pl.ds(4 + j, 1), :] = mean[:, j * B : (j + 1) * B]
        stat_in[t, mine] = stat_out[t]
        for d in range(15):
            pltpu.make_async_remote_copy(
                src_ref=stat_out.at[t], dst_ref=stat_in.at[t, mine], send_sem=ss.at[t, d], recv_sem=sr.at[t, d],
                device_id=plane_dev[d], device_id_type=MESH,
            ).start()
        return carry

    lax.fori_loop(0, 4, finish, 0)

    for zz in range(8):
        ktb[zz] = kb[pl.ds(2 * zz, 2)].reshape(2 * B, B).T

    def weigh(t, carry):
        top, mean = tops[t, 0:1, :], tops[t, 1:2, :]

        def step(i, carry):
            for zz in (2 * i, 2 * i + 1):
                w = jnp.exp2(s_buf[t, zz] - top)
                w_buf[t, zz] = w.astype(BF16)
                e_buf[t, zz] = (w * (dp_buf[t, zz] - mean)).astype(BF16)
            return carry

        return lax.fori_loop(0, 4, step, carry)

    lax.fori_loop(0, 4, weigh, 0)

    def combine(t, carry):
        for d in range(15):
            copy = pltpu.make_async_remote_copy(
                src_ref=stat_out.at[t], dst_ref=stat_in.at[t, lax.rem(mine + 15 - d, 16)], send_sem=ss.at[t, d],
                recv_sem=sr.at[t, d], device_id=plane_dev[d], device_id_type=MESH,
            )
            copy.wait_recv()
            copy.wait_send()
        level = stat_in[t, :, 0:4, :]
        mean = stat_in[t, :, 4:8, :]
        top = jnp.max(level, axis=0)
        e = jnp.exp2(level - top[None])
        total = jnp.sum(e, axis=0)
        lse = top + jnp.log(total) * LOG2E
        delta = jnp.sum(e * mean, axis=0) / total
        for j in range(4):
            here = slice(j * B, (j + 1) * B)
            f = jnp.exp2(tops[t, 0:1, here] - lse[j : j + 1])
            h = (tops[t, 1:2, here] - delta[j : j + 1]) * f
            factor[0, pl.ds(4 * t + j, 1), :] = f
            factor[1, pl.ds(4 * t + j, 1), :] = h
        return carry

    lax.fori_loop(0, 4, combine, 0)

    column = lambda i: up4(x, (2, 1, 3, 0)[i])

    def q_copy(i, j):
        return pltpu.make_async_remote_copy(
            src_ref=q_out.at[i, up4(y, j)], dst_ref=q_in.at[i, j], send_sem=qs_sem.at[i, j], recv_sem=qr_sem.at[i, j],
            device_id=device(column(i), up4(y, j), z, c), device_id_type=MESH,
        )

    def query_side(i):
        t = column(i)
        of_e = nn(ktb[0], e_buf[t, 0])
        of_w = nn(ktb[0], w_buf[t, 0])
        for zz in range(1, 8):
            of_e += nn(ktb[zz], e_buf[t, zz])
            of_w += nn(ktb[zz], w_buf[t, zz])
        for j in range(4):
            here = slice(j * B, (j + 1) * B)
            f = factor[0, pl.ds(4 * t + j, 1), :]
            h = factor[1, pl.ds(4 * t + j, 1), :]
            q_out[i, j] = (of_e[:, here] * f + of_w[:, here] * h).astype(BF16)
        for j in (2, 1, 3, 0):
            if (i, j) != (3, 0):
                q_copy(i, j).start()

    f_col, h_col = factor[0].T, factor[1].T
    for s in range(16):
        f, h = f_col[:, s : s + 1], h_col[:, s : s + 1]
        rows = qb[s].astype(F32)
        q_scaled[s] = (rows * f).astype(BF16)
        g_scaled[s, :, :B] = (gb[s].astype(F32) * f).astype(BF16)
        g_scaled[s, :, B:] = (rows * h).astype(BF16)

    def pair_copy(off):
        return pltpu.make_async_remote_copy(
            src_ref=pair_out.at[off], dst_ref=pair_in.at[off], send_sem=ps.at[off], recv_sem=pr.at[off],
            device_id=to_pair, device_id_type=MESH,
        )

    to_z = lambda d: device(x, y, up8(z, d), c)

    def z_copy(n, src, dst, d):
        return pltpu.make_async_remote_copy(
            src_ref=src, dst_ref=dst, send_sem=zs.at[n], recv_sem=zr.at[n], device_id=to_z(d), device_id_type=MESH
        )

    hops = {
        4: (z_copy(0, z_out.at[4, 0], z_in.at[0, 0], 2), z_copy(1, z_out.at[4, 1], z_in.at[0, 1], 6)),
        3: (z_copy(2, z_out.at[3], z_in.at[1], 1),),
        5: (z_copy(3, z_out.at[5], z_in.at[2], 7),),
        2: (z_copy(4, z_out.at[2], z_in.at[3], 2),),
        6: (z_copy(5, z_out.at[6], z_in.at[4], 6),),
        1: (z_copy(6, z_out.at[1], z_in.at[5], 1),),
        7: (z_copy(7, z_out.at[7], z_in.at[6], 7),),
    }

    def pass_on(off):
        pair_copy(off).wait_recv()
        for w in range(2):
            total = part[off, w] + pair_in[off, w].astype(F32)
            if off in (2, 6):
                if w == 0:
                    hops[3 if off == 2 else 5][0].wait_recv()
                total += z_in[1 if off == 2 else 2, w].astype(F32)
                if w == (0 if off == 2 else 1):
                    hops[4][w].wait_recv()
                    total += z_in[0, w].astype(F32)
            z_out[off, w] = total.astype(BF16)
        for copy in hops[off]:
            copy.start()

    def key_side(off):
        zz = up8(z, off)
        dk = jnp.zeros((2 * B, B), F32)
        dvk = jnp.zeros((2 * B, 2 * B), F32)
        for t in range(4):
            dk += nn(e_buf[t, zz], q_scaled[4 * t : 4 * t + 4].reshape(4 * B, B))
            dvk += nn(w_buf[t, zz], g_scaled[4 * t : 4 * t + 4].reshape(4 * B, 2 * B))
        for w, total in enumerate((dk + dvk[:, B:], dvk[:, :B])):
            tmp[w] = total.reshape(2, B, B)
            part[off, w] = tmp[w, c]
            pair_out[off, w] = tmp[w, other].astype(BF16)
        pair_copy(off).start()

    key_side(4)
    key_side(3)
    pass_on(4)
    key_side(5)
    pass_on(3)
    query_side(0)
    pass_on(5)
    key_side(2)
    key_side(6)
    query_side(1)
    pass_on(2)
    query_side(2)
    query_side(3)
    pass_on(6)
    key_side(1)
    key_side(7)
    pass_on(1)
    key_side(0)
    pass_on(7)

    scale = 1.0 / math.sqrt(B)
    own = q_out[3, y].astype(F32)
    for i in range(4):
        for j in range(4):
            if (i, j) != (3, 0):
                q_copy(i, j).wait_recv()
                own += q_in[i, j].astype(F32)
    out_ref[0] = (own * scale).T.astype(BF16)

    pair_copy(0).wait_recv()
    acc = [part[0, w] + pair_in[0, w].astype(F32) for w in range(2)]
    for off, n in ((2, 3), (6, 4), (1, 5), (7, 6)):
        hops[off][0].wait_recv()
        for w in range(2):
            acc[w] += z_in[n, w].astype(F32)
    out_ref[1] = (acc[0] * scale).astype(BF16)
    out_ref[2] = acc[1].astype(BF16)

    for copy in sent:
        copy.wait_send()
    for off in range(8):
        pair_copy(off).wait_send()
        for copy in hops.get(off, ()):
            copy.wait_send()
    for i in range(4):
        for j in range(4):
            if (i, j) != (3, 0):
                q_copy(i, j).wait_send()


def body(queries, key_rows, value_rows, grad_output, positions):
    vmem = pl.BlockSpec(memory_space=pltpu.VMEM)
    hbm = pl.BlockSpec(memory_space=pl.ANY)
    dma = pltpu.SemaphoreType.DMA
    blocks = pltpu.VMEM((16, B, B), BF16)
    grads = pl.pallas_call(
        kernel,
        out_shape=jax.ShapeDtypeStruct((3, B, B), BF16),
        in_specs=[hbm] * 5,
        out_specs=vmem,
        scratch_shapes=[
            blocks, blocks, blocks, blocks,
            pltpu.VMEM((256, B), jnp.int32),
            pltpu.VMEM((8, B, 2 * B), BF16),
            pltpu.VMEM((16, B, B), F32),
            pltpu.VMEM((16, B), F32),
            pltpu.VMEM((4, 8, 2 * B, 4 * B), F32),
            pltpu.VMEM((4, 8, 2 * B, 4 * B), F32),
            pltpu.VMEM((4, 8, 4 * B), F32),
            pltpu.VMEM((4, 8, 4 * B), F32),
            pltpu.VMEM((4, 8, 4 * B), F32),
            pltpu.VMEM((4, 8, B), F32),
            pltpu.VMEM((4, 16, 8, B), F32),
            pltpu.VMEM((2, 16, B), F32),
            pltpu.VMEM((4, 8, 4 * B), F32),
            pltpu.VMEM((4, 8, 2 * B, 4 * B), BF16),
            pltpu.VMEM((4, 8, 2 * B, 4 * B), BF16),
            pltpu.VMEM((16, B, B), BF16),
            pltpu.VMEM((16, B, 2 * B), BF16),
            pltpu.VMEM((8, 2, B, B), F32),
            pltpu.VMEM((2, 2, B, B), F32),
            pltpu.VMEM((8, 2, B, B), BF16),
            pltpu.VMEM((8, 2, B, B), BF16),
            pltpu.VMEM((8, 2, B, B), BF16),
            pltpu.VMEM((7, 2, B, B), BF16),
            pltpu.VMEM((4, 4, B, B), BF16),
            pltpu.VMEM((4, 4, B, B), BF16),
            dma((5,)),
            dma((60,)), dma((60,)),
            dma((4, 15)), dma((4, 15)),
            dma((8,)), dma((8,)),
            dma((8,)), dma((8,)),
            dma((4, 4)), dma((4, 4)),
        ],
        compiler_params=pltpu.CompilerParams(
            collective_id=0, has_side_effects=True, vmem_limit_bytes=63 * 1024 * 1024
        ),
        name="attention_backward",
    )(queries, key_rows, value_rows, grad_output, positions.reshape(-1, B))
    return grads[0], grads[1], grads[2]


def solution(mesh):
    spec = P(("row", "col"), None)
    return jax.shard_map(
        body,
        mesh=mesh,
        in_specs=(spec, spec, spec, spec, P()),
        out_specs=(spec, spec, spec),
        check_vma=False,
    )
```

```python
import math

import jax
import jax.numpy as jnp
from jax import lax
from jax.experimental import pallas as pl
from jax.experimental.pallas import tpu as pltpu
from jax.sharding import PartitionSpec as P

MESH = pl.DeviceIdType.MESH
F32 = jnp.float32
BF16 = jnp.bfloat16
B = 128
NEG = -1e30
FLOOR = -1e6
LOG2E = math.log2(math.e)


def device(x, y, z, c):
    return (y * 2 + lax.rem(z, 2), (x * 4 + lax.div(z, 2)) * 2 + c)


def nt(a, b):
    return lax.dot_general(a, b, (((1,), (1,)), ((), ())), preferred_element_type=F32)


def nn(a, b):
    return jnp.dot(a, b, preferred_element_type=F32)


def kernel(
    q_ref, k_ref, v_ref, g_ref, pos_hbm, out_ref,
    qb, gb, kvb, pos_ref, ktb, posk, posq, s_buf, dp_buf, mt, zt, dt, stat_out, stat_in, factor, tops,
    w_buf, e_buf, q_scaled, g_scaled, part, tmp, pair_out, pair_in, z_out, z_in, q_out, q_in,
    ins, gs, gr, ss, sr, ps, pr, zs, zr, qs_sem, qr_sem,
):
    row, col = lax.axis_index("row"), lax.axis_index("col")
    y, zlo = lax.div(row, 2), lax.rem(row, 2)
    x, c = lax.div(col, 8), lax.rem(col, 2)
    z = lax.rem(lax.div(col, 2), 4) * 2 + zlo
    up4 = lambda a, d: lax.rem(a + d, 4)
    up8 = lambda a, d: lax.rem(a + d, 8)
    other = 1 - c
    mine = x * 4 + y
    chip_scale = LOG2E / math.sqrt(B)

    here_k = z * 2 + c
    fetch = [
        pltpu.make_async_copy(src, dst, ins.at[n])
        for src, dst, n in (
            (
                (k_ref, kvb.at[here_k, 0], 0),
                (v_ref, kvb.at[here_k, 1], 0),
                (q_ref, qb.at[mine], 0),
                (g_ref, gb.at[mine], 0),
                (pos_hbm, pos_ref, 1),
            )
        )
    ]
    for copy in fetch:
        copy.start()

    plane = [lax.rem(mine + d, 16) for d in range(1, 16)]
    plane_dev = [device(lax.div(s, 4), lax.rem(s, 4), z, c) for s in plane]
    barrier = pltpu.get_barrier_semaphore()
    peers = [device(up4(x, d), y, z, c) for d in (2, 1, 3)] + [device(x, up4(y, d), z, c) for d in (2, 1, 3)]
    peers += [device(x, y, up8(z, d), c) for d in (2, 6, 1, 7)] + [device(x, y, z, other)]
    for p in peers:
        pl.semaphore_signal(barrier, inc=1, device_id=p, device_id_type=MESH)
    pltpu.make_async_copy(qb.at[0:4], qb.at[0:4], ins.at[0]).wait()
    pl.semaphore_wait(barrier, len(peers))

    to_pair = device(x, y, z, other)

    def whole(ref, send_sem, recv_sem):
        return pltpu.make_async_remote_copy(
            src_ref=ref, dst_ref=ref, send_sem=send_sem, recv_sem=recv_sem, device_id=to_pair, device_id_type=MESH
        )

    def send(src, to, n):
        pltpu.make_async_remote_copy(
            src_ref=src, dst_ref=src, send_sem=gs.at[0], recv_sem=gr.at[n], device_id=to, device_id_type=MESH
        ).start()

    done = set()

    def need(n, ref):
        if n not in done:
            done.add(n)
            whole(ref, gs.at[0], gr.at[n]).wait_recv()

    slot = lambda a, b: a * 4 + b
    xr, xl, yr, yl = up4(x, 1), up4(x, 3), up4(y, 1), up4(y, 3)
    x2, y2 = up4(x, 2), up4(y, 2)
    to_xr, to_xl = device(xr, y, z, c), device(xl, y, z, c)
    to_yr, to_yl = device(x, yr, z, c), device(x, yl, z, c)
    to_x2, to_y2 = device(x2, y, z, c), device(x, y2, z, c)
    plans = (
        (16, qb, lambda i, j: slot(i, j), x, y, (xl, xr, x2), (to_xr, to_xl, to_x2), (to_yr, to_yl, to_y2)),
        (19, gb, lambda i, j: slot(j, i), y, x, (yl, yr, y2), (to_yr, to_yl, to_y2), (to_xr, to_xl, to_x2)),
    )
    kv_at = lambda off: kvb.at[up8(z, off) * 2 + c]
    up = lambda d: device(x, y, up8(z, d), c)

    def send_across(p, n, src):
        to_b = plans[p][-1]
        for m in (2, 0, 1):
            send(src, to_b[m], 22 + (n if p == 0 else m))

    def send_pair(off):
        if off == 4:
            need(4, kv_at(4).at[0])
            need(0, kv_at(4).at[1])
        elif off:
            need(off, kv_at(off))
        send(kv_at(off), to_pair, 8 + off)

    def need_pair(*offs):
        for off in offs:
            need(8 + off, kv_at(off))

    send(kv_at(0), up(2), 6)
    send(kv_at(0), up(6), 2)
    for p, (first, buf, at, a, b, ias, to_a, to_b) in enumerate(plans):
        src = buf.at[at(a, b)]
        for n in (2, 0, 1):
            send(src, to_a[n], first + n)
        send_across(p, 3, src)
    send(kv_at(0), up(1), 7)
    send(kv_at(0), up(7), 1)
    send_pair(0)

    fetch[4].wait()
    zhi_col = lax.div(z, 2) * 2 + c
    for s in range(16):
        i, j = s // 4, s % 4
        posq[pl.ds(s, 1), :] = pos_ref[pl.ds((j * 2 + zlo) * 32 + i * 8 + zhi_col, 1), :].astype(F32)
    for s in range(16):
        zz, cc = s // 2, s % 2
        line = pos_ref[pl.ds((y * 2 + zz % 2) * 32 + (x * 4 + zz // 2) * 2 + cc, 1), :].astype(F32)
        posk[s] = jnp.broadcast_to(line, (B, B)).T

    def tile(t, zz):
        q_tile = qb[pl.ds(4 * t, 4)].reshape(4 * B, B)
        g_tile = gb[pl.ds(4 * t, 4)].reshape(4 * B, B)
        k_tile = kvb[pl.ds(2 * zz, 2), 0].reshape(2 * B, B)
        v_tile = kvb[pl.ds(2 * zz, 2), 1].reshape(2 * B, B)
        pq = jnp.concatenate([posq[pl.ds(4 * t + j, 1), :] for j in range(4)], axis=1)
        pk = posk[pl.ds(2 * zz, 2)].reshape(2 * B, B)
        pk = jnp.concatenate([pk] * 4, axis=1)
        s = jnp.where(pq >= pk, nt(k_tile, q_tile) * chip_scale, NEG)
        s_buf[t, zz] = s
        m = jnp.maximum(jnp.max(s, axis=0, keepdims=True), FLOOR)
        dp = nt(v_tile, g_tile)
        dp_buf[t, zz] = dp
        w = jnp.exp2(s - m)
        mt[t, pl.ds(zz, 1), :] = m
        zt[t, pl.ds(zz, 1), :] = jnp.sum(w, axis=0, keepdims=True)
        dt[t, pl.ds(zz, 1), :] = jnp.sum(w * dp, axis=0, keepdims=True)

    def tiles(n, pick):
        def step(i, carry):
            for t, zz in pick(i):
                tile(t, zz)
            return carry

        lax.fori_loop(0, n, step, 0)

    near = lambda i: up8(z, i + 5 * lax.div(i, 2))
    both = lambda i, d: up8(z, d + i * (8 - 2 * d))

    def across(n):
        for p, (first, buf, at, a, b, ias, to_a, to_b) in enumerate(plans):
            src = buf.at[at(ias[n], b)]
            need(first + n, src)
            send_across(p, n, src)

    across(0)
    across(1)
    need(6, kv_at(6))
    send(kv_at(6).at[0], up(2), 4)
    send(kv_at(6), up(1), 5)
    need(2, kv_at(2))
    send(kv_at(2).at[1], up(6), 0)
    send(kv_at(2), up(7), 3)
    across(2)
    for off in (1, 7, 2, 6):
        send_pair(off)

    def need_column(n):
        need(22 + n, qb.at[0 : 7 if n < 3 else 3])

    need_column(3)
    need_pair(0, 1, 7)
    tiles(3, lambda i: [(x, near(i))])
    need_pair(2, 6)
    tiles(1, lambda i: [(x, both(0, 2)), (x, both(1, 2))])
    need_column(0)
    need_column(1)
    tiles(3, lambda i: [(xl, near(i)), (xr, near(i))])
    for off in (3, 5, 4):
        send_pair(off)
    tiles(2, lambda i: [(xl, both(i, 2)), (xr, both(i, 2))])
    need_column(2)
    tiles(3, lambda i: [(x2, near(i))])
    tiles(1, lambda i: [(x2, both(0, 2)), (x2, both(1, 2))])
    need_pair(3, 5)
    tiles(4, lambda i: [(i, both(0, 3)), (i, both(1, 3))])
    need_pair(4)

    def finish(t, carry):
        tile(t, up8(z, 4))
        maxes = mt[t]
        top = jnp.max(maxes, axis=0, keepdims=True)
        tops[t, 0:1, :] = top
        f = jnp.exp2(maxes - top)
        total = jnp.sum(zt[t] * f, axis=0, keepdims=True)
        dot = jnp.sum(dt[t] * f, axis=0, keepdims=True)
        some = total > 0.0
        safe = jnp.where(some, total, 1.0)
        level = jnp.where(some, top + jnp.log(safe) * LOG2E, NEG)
        mean = dot / safe
        tops[t, 1:2, :] = mean
        for j in range(4):
            stat_out[t, pl.ds(j, 1), :] = level[:, j * B : (j + 1) * B]
            stat_out[t, pl.ds(4 + j, 1), :] = mean[:, j * B : (j + 1) * B]
        stat_in[t, mine] = stat_out[t]
        for d in range(15):
            pltpu.make_async_remote_copy(
                src_ref=stat_out.at[t], dst_ref=stat_in.at[t, mine], send_sem=ss.at[0], recv_sem=sr.at[t],
                device_id=plane_dev[d], device_id_type=MESH,
            ).start()
        return carry

    lax.fori_loop(0, 4, finish, 0)

    for zz in range(8):
        ktb[zz] = kvb[pl.ds(2 * zz, 2), 0].reshape(2 * B, B).T

    def weigh(t, carry):
        top, mean = tops[t, 0:1, :], tops[t, 1:2, :]

        def step(i, carry):
            for zz in (2 * i, 2 * i + 1):
                w = jnp.exp2(s_buf[t, zz] - top)
                w_buf[t, zz] = w.astype(BF16)
                e_buf[t, zz] = (w * (dp_buf[t, zz] - mean)).astype(BF16)
            return carry

        return lax.fori_loop(0, 4, step, carry)

    lax.fori_loop(0, 4, weigh, 0)

    def combine(t, carry):
        whole(stat_in.at[t, 0:15], ss.at[0], sr.at[t]).wait_recv()
        level = stat_in[t, :, 0:4, :]
        mean = stat_in[t, :, 4:8, :]
        top = jnp.max(level, axis=0)
        e = jnp.exp2(level - top[None])
        total = jnp.sum(e, axis=0)
        lse = top + jnp.log(total) * LOG2E
        delta = jnp.sum(e * mean, axis=0) / total
        for j in range(4):
            here = slice(j * B, (j + 1) * B)
            f = jnp.exp2(tops[t, 0:1, here] - lse[j : j + 1])
            h = (tops[t, 1:2, here] - delta[j : j + 1]) * f
            factor[0, pl.ds(4 * t + j, 1), :] = f
            factor[1, pl.ds(4 * t + j, 1), :] = h
        return carry

    lax.fori_loop(0, 4, combine, 0)

    column = lambda i: up4(x, (2, 1, 3, 0)[i])

    def q_copy(i, j):
        return pltpu.make_async_remote_copy(
            src_ref=q_out.at[4 * i + up4(y, j)], dst_ref=q_in.at[4 * i + j], send_sem=qs_sem.at[0], recv_sem=qr_sem.at[0],
            device_id=device(column(i), up4(y, j), z, c), device_id_type=MESH,
        )

    def query_side(i):
        t = column(i)
        of_e = nn(ktb[0], e_buf[t, 0])
        of_w = nn(ktb[0], w_buf[t, 0])
        for zz in range(1, 8):
            of_e += nn(ktb[zz], e_buf[t, zz])
            of_w += nn(ktb[zz], w_buf[t, zz])
        for j in range(4):
            here = slice(j * B, (j + 1) * B)
            f = factor[0, pl.ds(4 * t + j, 1), :]
            h = factor[1, pl.ds(4 * t + j, 1), :]
            q_out[4 * i + j] = (of_e[:, here] * f + of_w[:, here] * h).astype(BF16)
        for j in (2, 1, 3, 0):
            if (i, j) != (3, 0):
                q_copy(i, j).start()

    f_col, h_col = factor[0].T, factor[1].T
    for s in range(16):
        f, h = f_col[:, s : s + 1], h_col[:, s : s + 1]
        rows = qb[s].astype(F32)
        q_scaled[s] = (rows * f).astype(BF16)
        g_scaled[s, :, :B] = (gb[s].astype(F32) * f).astype(BF16)
        g_scaled[s, :, B:] = (rows * h).astype(BF16)

    def pair_copy(off):
        return pltpu.make_async_remote_copy(
            src_ref=pair_out.at[off], dst_ref=pair_in.at[off], send_sem=ps.at[0], recv_sem=pr.at[off],
            device_id=to_pair, device_id_type=MESH,
        )

    to_z = lambda d: device(x, y, up8(z, d), c)

    def z_copy(n, src, dst, d):
        return pltpu.make_async_remote_copy(
            src_ref=src, dst_ref=dst, send_sem=zs.at[0], recv_sem=zr.at[n], device_id=to_z(d), device_id_type=MESH
        )

    hops = {
        4: (z_copy(0, z_out.at[4, 0], z_in.at[0, 0], 2), z_copy(1, z_out.at[4, 1], z_in.at[0, 1], 6)),
        3: (z_copy(2, z_out.at[3], z_in.at[1], 1),),
        5: (z_copy(3, z_out.at[5], z_in.at[2], 7),),
        2: (z_copy(4, z_out.at[2], z_in.at[3], 2),),
        6: (z_copy(5, z_out.at[6], z_in.at[4], 6),),
        1: (z_copy(6, z_out.at[1], z_in.at[5], 1),),
        7: (z_copy(7, z_out.at[7], z_in.at[6], 7),),
    }

    def pass_on(off):
        pair_copy(off).wait_recv()
        for w in range(2):
            total = part[off, w] + pair_in[off, w].astype(F32)
            if off in (2, 6):
                if w == 0:
                    hops[3 if off == 2 else 5][0].wait_recv()
                total += z_in[1 if off == 2 else 2, w].astype(F32)
                if w == (0 if off == 2 else 1):
                    hops[4][w].wait_recv()
                    total += z_in[0, w].astype(F32)
            z_out[off, w] = total.astype(BF16)
        for copy in hops[off]:
            copy.start()

    def key_side(off):
        zz = up8(z, off)
        dk = jnp.zeros((2 * B, B), F32)
        dvk = jnp.zeros((2 * B, 2 * B), F32)
        for t in range(4):
            dk += nn(e_buf[t, zz], q_scaled[4 * t : 4 * t + 4].reshape(4 * B, B))
            dvk += nn(w_buf[t, zz], g_scaled[4 * t : 4 * t + 4].reshape(4 * B, 2 * B))
        for w, total in enumerate((dk + dvk[:, B:], dvk[:, :B])):
            tmp[w] = total.reshape(2, B, B)
            part[off, w] = tmp[w, c]
            pair_out[off, w] = tmp[w, other].astype(BF16)
        pair_copy(off).start()

    key_side(4)
    key_side(3)
    key_side(5)
    key_side(2)
    pass_on(4)
    key_side(6)
    pass_on(3)
    query_side(0)
    pass_on(5)
    query_side(1)
    query_side(2)
    query_side(3)
    key_side(1)
    key_side(7)
    key_side(0)
    pass_on(2)
    pass_on(6)
    pass_on(1)
    pass_on(7)

    scale = 1.0 / math.sqrt(B)
    pair_copy(0).wait_recv()
    acc = [part[0, w] + pair_in[0, w].astype(F32) for w in range(2)]
    own = q_out[12 + y].astype(F32)
    whole(q_in.at[0:15], qs_sem.at[0], qr_sem.at[0]).wait_recv()
    for n in range(16):
        if n != 12:
            own += q_in[n].astype(F32)
    out_ref[0] = (own * scale).T.astype(BF16)
    for off, n in ((1, 5), (7, 6), (2, 3), (6, 4)):
        hops[off][0].wait_recv()
        for w in range(2):
            acc[w] += z_in[n, w].astype(F32)
    out_ref[1] = (acc[0] * scale).astype(BF16)
    out_ref[2] = acc[1].astype(BF16)

    whole(s_buf.at[0, 0:5, 0:192, :], gs.at[0], gr.at[0]).wait_send()
    whole(stat_in.at[:, 0:15], ss.at[0], sr.at[0]).wait_send()
    whole(pair_out, ps.at[0], pr.at[0]).wait_send()
    whole(z_out.at[1:8], zs.at[0], zr.at[0]).wait_send()
    whole(q_in.at[0:15], qs_sem.at[0], qr_sem.at[0]).wait_send()


def body(queries, key_rows, value_rows, grad_output, positions):
    vmem = pl.BlockSpec(memory_space=pltpu.VMEM)
    hbm = pl.BlockSpec(memory_space=pl.ANY)
    dma = pltpu.SemaphoreType.DMA
    blocks = pltpu.VMEM((16, B, B), BF16)
    grads = pl.pallas_call(
        kernel,
        out_shape=jax.ShapeDtypeStruct((3, B, B), BF16),
        in_specs=[hbm] * 5,
        out_specs=vmem,
        scratch_shapes=[
            blocks, blocks,
            pltpu.VMEM((16, 2, B, B), BF16),
            pltpu.VMEM((256, B), jnp.int32),
            pltpu.VMEM((8, B, 2 * B), BF16),
            pltpu.VMEM((16, B, B), F32),
            pltpu.VMEM((16, B), F32),
            pltpu.VMEM((4, 8, 2 * B, 4 * B), F32),
            pltpu.VMEM((4, 8, 2 * B, 4 * B), F32),
            pltpu.VMEM((4, 8, 4 * B), F32),
            pltpu.VMEM((4, 8, 4 * B), F32),
            pltpu.VMEM((4, 8, 4 * B), F32),
            pltpu.VMEM((4, 8, B), F32),
            pltpu.VMEM((4, 16, 8, B), F32),
            pltpu.VMEM((2, 16, B), F32),
            pltpu.VMEM((4, 8, 4 * B), F32),
            pltpu.VMEM((4, 8, 2 * B, 4 * B), BF16),
            pltpu.VMEM((4, 8, 2 * B, 4 * B), BF16),
            pltpu.VMEM((16, B, B), BF16),
            pltpu.VMEM((16, B, 2 * B), BF16),
            pltpu.VMEM((8, 2, B, B), F32),
            pltpu.VMEM((2, 2, B, B), F32),
            pltpu.VMEM((8, 2, B, B), BF16),
            pltpu.VMEM((8, 2, B, B), BF16),
            pltpu.VMEM((8, 2, B, B), BF16),
            pltpu.VMEM((7, 2, B, B), BF16),
            blocks, blocks,
            dma((2,)),
            dma((1,)), dma((26,)),
            dma((1,)), dma((4,)),
            dma((1,)), dma((8,)),
            dma((1,)), dma((8,)),
            dma((1,)), dma((1,)),
        ],
        compiler_params=pltpu.CompilerParams(
            collective_id=0, has_side_effects=True, vmem_limit_bytes=63 * 1024 * 1024
        ),
        name="attention_backward",
    )(queries, key_rows, value_rows, grad_output, positions.reshape(-1, B))
    return grads[0], grads[1], grads[2]


def solution(mesh):
    spec = P(("row", "col"), None)
    return jax.shard_map(
        body,
        mesh=mesh,
        in_specs=(spec, spec, spec, spec, P()),
        out_specs=(spec, spec, spec),
        check_vma=False,
    )
```

```python
import math

import jax
import jax.numpy as jnp
from jax import lax
from jax.experimental import pallas as pl
from jax.experimental.pallas import tpu as pltpu
from jax.sharding import PartitionSpec as P

MESH = pl.DeviceIdType.MESH
F32 = jnp.float32
BF16 = jnp.bfloat16
B = 128
NEG = -1e30
FLOOR = -1e6
LOG2E = math.log2(math.e)


def device(x, y, z, c):
    return (y * 2 + lax.rem(z, 2), (x * 4 + lax.div(z, 2)) * 2 + c)


def nt(a, b):
    return lax.dot_general(a, b, (((1,), (1,)), ((), ())), preferred_element_type=F32)


def nn(a, b):
    return jnp.dot(a, b, preferred_element_type=F32)


def kernel(
    q_ref, k_ref, v_ref, g_ref, pos_hbm, out_ref,
    qb, gb, kvb, pos_ref, ktb, posk, posq, s_buf, dp_buf, mt, zt, dt, stat_out, stat_in, factor, tops,
    w_buf, e_buf, sums, q_scaled, g_scaled, part, tmp, pair_out, pair_in, z_out, z_in, q_out, q_in,
    ins, gs, gr, ss, sr, ps, pr, zs, zr, qs_sem, qr_sem,
):
    row, col = lax.axis_index("row"), lax.axis_index("col")
    y, zlo = lax.div(row, 2), lax.rem(row, 2)
    x, c = lax.div(col, 8), lax.rem(col, 2)
    z = lax.rem(lax.div(col, 2), 4) * 2 + zlo
    up4 = lambda a, d: lax.rem(a + d, 4)
    up8 = lambda a, d: lax.rem(a + d, 8)
    other = 1 - c
    mine = x * 4 + y
    chip_scale = LOG2E / math.sqrt(B)

    here_k = z * 2 + c
    fetch = [
        pltpu.make_async_copy(src, dst, ins.at[n])
        for src, dst, n in (
            (
                (k_ref, kvb.at[here_k, 0], 0),
                (v_ref, kvb.at[here_k, 1], 0),
                (q_ref, qb.at[mine], 0),
                (g_ref, gb.at[mine], 0),
                (pos_hbm, pos_ref, 1),
            )
        )
    ]
    for copy in fetch:
        copy.start()

    plane = [lax.rem(mine + d, 16) for d in range(1, 16)]
    plane_dev = [device(lax.div(s, 4), lax.rem(s, 4), z, c) for s in plane]
    barrier = pltpu.get_barrier_semaphore()
    peers = [device(up4(x, d), y, z, c) for d in (2, 1, 3)] + [device(x, up4(y, d), z, c) for d in (2, 1, 3)]
    peers += [device(x, y, up8(z, d), c) for d in (2, 6, 1, 7)] + [device(x, y, z, other)]
    for p in peers:
        pl.semaphore_signal(barrier, inc=1, device_id=p, device_id_type=MESH)
    pltpu.make_async_copy(qb.at[0:4], qb.at[0:4], ins.at[0]).wait()
    pl.semaphore_wait(barrier, len(peers))

    to_pair = device(x, y, z, other)

    def whole(ref, send_sem, recv_sem):
        return pltpu.make_async_remote_copy(
            src_ref=ref, dst_ref=ref, send_sem=send_sem, recv_sem=recv_sem, device_id=to_pair, device_id_type=MESH
        )

    def send(src, to, n):
        pltpu.make_async_remote_copy(
            src_ref=src, dst_ref=src, send_sem=gs.at[0], recv_sem=gr.at[n], device_id=to, device_id_type=MESH
        ).start()

    done = set()

    def need(n, ref):
        if n not in done:
            done.add(n)
            whole(ref, gs.at[0], gr.at[n]).wait_recv()

    slot = lambda a, b: a * 4 + b
    xr, xl, yr, yl = up4(x, 1), up4(x, 3), up4(y, 1), up4(y, 3)
    x2, y2 = up4(x, 2), up4(y, 2)
    to_xr, to_xl = device(xr, y, z, c), device(xl, y, z, c)
    to_yr, to_yl = device(x, yr, z, c), device(x, yl, z, c)
    to_x2, to_y2 = device(x2, y, z, c), device(x, y2, z, c)
    plans = (
        (16, qb, lambda i, j: slot(i, j), x, y, (xl, xr, x2), (to_xr, to_xl, to_x2), (to_yr, to_yl, to_y2)),
        (19, gb, lambda i, j: slot(j, i), y, x, (yl, yr, y2), (to_yr, to_yl, to_y2), (to_xr, to_xl, to_x2)),
    )
    kv_at = lambda off: kvb.at[up8(z, off) * 2 + c]
    up = lambda d: device(x, y, up8(z, d), c)

    def send_across(p, n, src):
        to_b = plans[p][-1]
        for m in (2, 0, 1):
            send(src, to_b[m], 22 + (n if p == 0 else m))

    def send_pair(off):
        if off == 4:
            need(4, kv_at(4).at[0])
            need(0, kv_at(4).at[1])
        elif off:
            need(off, kv_at(off))
        send(kv_at(off), to_pair, 8 + off)

    def need_pair(*offs):
        for off in offs:
            need(8 + off, kv_at(off))

    send(kv_at(0), up(2), 6)
    send(kv_at(0), up(6), 2)
    for p, (first, buf, at, a, b, ias, to_a, to_b) in enumerate(plans):
        src = buf.at[at(a, b)]
        for n in (2, 0, 1):
            send(src, to_a[n], first + n)
        send_across(p, 3, src)
    send(kv_at(0), up(1), 7)
    send(kv_at(0), up(7), 1)
    send_pair(0)

    fetch[4].wait()
    zhi_col = lax.div(z, 2) * 2 + c
    for s in range(16):
        i, j = s // 4, s % 4
        posq[pl.ds(s, 1), :] = pos_ref[pl.ds((j * 2 + zlo) * 32 + i * 8 + zhi_col, 1), :].astype(F32)
    for s in range(16):
        zz, cc = s // 2, s % 2
        line = pos_ref[pl.ds((y * 2 + zz % 2) * 32 + (x * 4 + zz // 2) * 2 + cc, 1), :].astype(F32)
        posk[s] = jnp.broadcast_to(line, (B, B)).T

    def tile(t, zz):
        q_tile = qb[pl.ds(4 * t, 4)].reshape(4 * B, B)
        g_tile = gb[pl.ds(4 * t, 4)].reshape(4 * B, B)
        k_tile = kvb[pl.ds(2 * zz, 2), 0].reshape(2 * B, B)
        v_tile = kvb[pl.ds(2 * zz, 2), 1].reshape(2 * B, B)
        pq = jnp.concatenate([posq[pl.ds(4 * t + j, 1), :] for j in range(4)], axis=1)
        pk = posk[pl.ds(2 * zz, 2)].reshape(2 * B, B)
        pk = jnp.concatenate([pk] * 4, axis=1)
        s = jnp.where(pq >= pk, nt(k_tile, q_tile) * chip_scale, NEG)
        s_buf[t, zz] = s
        m = jnp.maximum(jnp.max(s, axis=0, keepdims=True), FLOOR)
        dp = nt(v_tile, g_tile)
        dp_buf[t, zz] = dp
        w = jnp.exp2(s - m)
        mt[t, pl.ds(zz, 1), :] = m
        zt[t, pl.ds(zz, 1), :] = jnp.sum(w, axis=0, keepdims=True)
        dt[t, pl.ds(zz, 1), :] = jnp.sum(w * dp, axis=0, keepdims=True)

    def tiles(n, pick):
        def step(i, carry):
            for t, zz in pick(i):
                tile(t, zz)
            return carry

        lax.fori_loop(0, n, step, 0)

    near = lambda i: up8(z, i + 5 * lax.div(i, 2))
    both = lambda i, d: up8(z, d + i * (8 - 2 * d))

    def across(n):
        for p, (first, buf, at, a, b, ias, to_a, to_b) in enumerate(plans):
            src = buf.at[at(ias[n], b)]
            need(first + n, src)
            send_across(p, n, src)

    across(0)
    across(1)
    need(6, kv_at(6))
    send(kv_at(6).at[0], up(2), 4)
    send(kv_at(6), up(1), 5)
    need(2, kv_at(2))
    send(kv_at(2).at[1], up(6), 0)
    send(kv_at(2), up(7), 3)
    across(2)
    for off in (1, 7, 2, 6):
        send_pair(off)

    def need_column(n):
        need(22 + n, qb.at[0 : 7 if n < 3 else 3])

    need_column(3)
    need_pair(0, 1, 7)
    tiles(3, lambda i: [(x, near(i))])
    need_pair(2, 6)
    tiles(1, lambda i: [(x, both(0, 2)), (x, both(1, 2))])
    need_column(0)
    need_column(1)
    tiles(3, lambda i: [(xl, near(i)), (xr, near(i))])
    for off in (3, 5, 4):
        send_pair(off)
    tiles(2, lambda i: [(xl, both(i, 2)), (xr, both(i, 2))])
    need_column(2)
    tiles(3, lambda i: [(x2, near(i))])
    tiles(1, lambda i: [(x2, both(0, 2)), (x2, both(1, 2))])
    need_pair(3, 5)
    tiles(4, lambda i: [(i, both(0, 3)), (i, both(1, 3))])
    need_pair(4)

    def finish(t, carry):
        tile(t, up8(z, 4))
        maxes = mt[t]
        top = jnp.max(maxes, axis=0, keepdims=True)
        tops[t, 0:1, :] = top
        f = jnp.exp2(maxes - top)
        total = jnp.sum(zt[t] * f, axis=0, keepdims=True)
        dot = jnp.sum(dt[t] * f, axis=0, keepdims=True)
        some = total > 0.0
        safe = jnp.where(some, total, 1.0)
        level = jnp.where(some, top + jnp.log(safe) * LOG2E, NEG)
        mean = dot / safe
        tops[t, 1:2, :] = mean
        for j in range(4):
            stat_out[t, pl.ds(j, 1), :] = level[:, j * B : (j + 1) * B]
            stat_out[t, pl.ds(4 + j, 1), :] = mean[:, j * B : (j + 1) * B]
        stat_in[t, mine] = stat_out[t]
        for d in range(15):
            pltpu.make_async_remote_copy(
                src_ref=stat_out.at[t], dst_ref=stat_in.at[t, mine], send_sem=ss.at[0], recv_sem=sr.at[t],
                device_id=plane_dev[d], device_id_type=MESH,
            ).start()
        return carry

    lax.fori_loop(0, 4, finish, 0)

    for zz in range(8):
        ktb[zz] = kvb[pl.ds(2 * zz, 2), 0].reshape(2 * B, B).T

    def weigh(t, carry):
        top, mean = tops[t, 0:1, :], tops[t, 1:2, :]
        of_e = of_w = None
        for zz in range(9):
            if zz < 8:
                w = jnp.exp2(s_buf[t, zz] - top)
                w_buf[t, zz] = w.astype(BF16)
                e_buf[t, zz] = (w * (dp_buf[t, zz] - mean)).astype(BF16)
            if zz:
                by_e, by_w = (nn(ktb[zz - 1], buf[t, zz - 1]) for buf in (e_buf, w_buf))
                of_e, of_w = (by_e, by_w) if zz == 1 else (of_e + by_e, of_w + by_w)
        sums[t, 0] = of_e
        sums[t, 1] = of_w
        return carry

    lax.fori_loop(0, 4, weigh, 0)

    def combine(t, carry):
        whole(stat_in.at[t, 0:15], ss.at[0], sr.at[t]).wait_recv()
        level = stat_in[t, :, 0:4, :]
        mean = stat_in[t, :, 4:8, :]
        top = jnp.max(level, axis=0)
        e = jnp.exp2(level - top[None])
        total = jnp.sum(e, axis=0)
        lse = top + jnp.log(total) * LOG2E
        delta = jnp.sum(e * mean, axis=0) / total
        for j in range(4):
            here = slice(j * B, (j + 1) * B)
            f = jnp.exp2(tops[t, 0:1, here] - lse[j : j + 1])
            h = (tops[t, 1:2, here] - delta[j : j + 1]) * f
            factor[0, pl.ds(4 * t + j, 1), :] = f
            factor[1, pl.ds(4 * t + j, 1), :] = h
        return carry

    lax.fori_loop(0, 4, combine, 0)

    column = lambda i: up4(x, (2, 1, 3, 0)[i])

    def q_copy(i, j):
        return pltpu.make_async_remote_copy(
            src_ref=q_out.at[4 * i + up4(y, j)], dst_ref=q_in.at[4 * i + j], send_sem=qs_sem.at[0], recv_sem=qr_sem.at[0],
            device_id=device(column(i), up4(y, j), z, c), device_id_type=MESH,
        )

    def query_side(i):
        t = column(i)
        for j in range(4):
            here = slice(j * B, (j + 1) * B)
            f = factor[0, pl.ds(4 * t + j, 1), :]
            h = factor[1, pl.ds(4 * t + j, 1), :]
            q_out[4 * i + j] = (sums[t, 0, :, here] * f + sums[t, 1, :, here] * h).astype(BF16)
        for j in (2, 1, 3, 0):
            if (i, j) != (3, 0):
                q_copy(i, j).start()

    f_col, h_col = factor[0].T, factor[1].T
    for s in range(16):
        f, h = f_col[:, s : s + 1], h_col[:, s : s + 1]
        rows = qb[s].astype(F32)
        q_scaled[s] = (rows * f).astype(BF16)
        g_scaled[s, :, :B] = (gb[s].astype(F32) * f).astype(BF16)
        g_scaled[s, :, B:] = (rows * h).astype(BF16)

    def pair_copy(off):
        return pltpu.make_async_remote_copy(
            src_ref=pair_out.at[off], dst_ref=pair_in.at[off], send_sem=ps.at[0], recv_sem=pr.at[off],
            device_id=to_pair, device_id_type=MESH,
        )

    to_z = lambda d: device(x, y, up8(z, d), c)

    def z_copy(n, src, dst, d):
        return pltpu.make_async_remote_copy(
            src_ref=src, dst_ref=dst, send_sem=zs.at[0], recv_sem=zr.at[n], device_id=to_z(d), device_id_type=MESH
        )

    hops = {
        4: (z_copy(0, z_out.at[4, 0], z_in.at[0, 0], 2), z_copy(1, z_out.at[4, 1], z_in.at[0, 1], 6)),
        3: (z_copy(2, z_out.at[3], z_in.at[1], 1),),
        5: (z_copy(3, z_out.at[5], z_in.at[2], 7),),
        2: (z_copy(4, z_out.at[2], z_in.at[3], 2),),
        6: (z_copy(5, z_out.at[6], z_in.at[4], 6),),
        1: (z_copy(6, z_out.at[1], z_in.at[5], 1),),
        7: (z_copy(7, z_out.at[7], z_in.at[6], 7),),
    }

    def pass_on(off):
        pair_copy(off).wait_recv()
        for w in range(2):
            total = part[off, w] + pair_in[off, w].astype(F32)
            if off in (2, 6):
                if w == 0:
                    hops[3 if off == 2 else 5][0].wait_recv()
                total += z_in[1 if off == 2 else 2, w].astype(F32)
                if w == (0 if off == 2 else 1):
                    hops[4][w].wait_recv()
                    total += z_in[0, w].astype(F32)
            z_out[off, w] = total.astype(BF16)
        for copy in hops[off]:
            copy.start()

    def key_side(off):
        zz = up8(z, off)
        dk = jnp.zeros((2 * B, B), F32)
        dvk = jnp.zeros((2 * B, 2 * B), F32)
        for t in range(4):
            dk += nn(e_buf[t, zz], q_scaled[4 * t : 4 * t + 4].reshape(4 * B, B))
            dvk += nn(w_buf[t, zz], g_scaled[4 * t : 4 * t + 4].reshape(4 * B, 2 * B))
        for w, total in enumerate((dk + dvk[:, B:], dvk[:, :B])):
            tmp[w] = total.reshape(2, B, B)
            part[off, w] = tmp[w, c]
            pair_out[off, w] = tmp[w, other].astype(BF16)
        pair_copy(off).start()

    key_side(4)
    query_side(0)
    key_side(3)
    query_side(1)
    key_side(5)
    query_side(2)
    query_side(3)
    key_side(1)
    pass_on(4)
    key_side(7)
    pass_on(3)
    key_side(2)
    pass_on(5)
    pass_on(1)
    key_side(6)
    pass_on(7)
    key_side(0)
    pass_on(2)
    pass_on(6)

    scale = 1.0 / math.sqrt(B)
    pair_copy(0).wait_recv()
    acc = [part[0, w] + pair_in[0, w].astype(F32) for w in range(2)]
    own = q_out[12 + y].astype(F32)
    whole(q_in.at[0:15], qs_sem.at[0], qr_sem.at[0]).wait_recv()
    for n in range(16):
        if n != 12:
            own += q_in[n].astype(F32)
    out_ref[0] = (own * scale).T.astype(BF16)
    for off, n in ((1, 5), (7, 6), (2, 3), (6, 4)):
        hops[off][0].wait_recv()
        for w in range(2):
            acc[w] += z_in[n, w].astype(F32)
    out_ref[1] = (acc[0] * scale).astype(BF16)
    out_ref[2] = acc[1].astype(BF16)

    whole(s_buf.at[0, 0:5, 0:192, :], gs.at[0], gr.at[0]).wait_send()
    whole(stat_in.at[:, 0:15], ss.at[0], sr.at[0]).wait_send()
    whole(pair_out, ps.at[0], pr.at[0]).wait_send()
    whole(z_out.at[1:8], zs.at[0], zr.at[0]).wait_send()
    whole(q_in.at[0:15], qs_sem.at[0], qr_sem.at[0]).wait_send()


def body(queries, key_rows, value_rows, grad_output, positions):
    vmem = pl.BlockSpec(memory_space=pltpu.VMEM)
    hbm = pl.BlockSpec(memory_space=pl.ANY)
    dma = pltpu.SemaphoreType.DMA
    blocks = pltpu.VMEM((16, B, B), BF16)
    grads = pl.pallas_call(
        kernel,
        out_shape=jax.ShapeDtypeStruct((3, B, B), BF16),
        in_specs=[hbm] * 5,
        out_specs=vmem,
        scratch_shapes=[
            blocks, blocks,
            pltpu.VMEM((16, 2, B, B), BF16),
            pltpu.VMEM((256, B), jnp.int32),
            pltpu.VMEM((8, B, 2 * B), BF16),
            pltpu.VMEM((16, B, B), F32),
            pltpu.VMEM((16, B), F32),
            pltpu.VMEM((4, 8, 2 * B, 4 * B), F32),
            pltpu.VMEM((4, 8, 2 * B, 4 * B), F32),
            pltpu.VMEM((4, 8, 4 * B), F32),
            pltpu.VMEM((4, 8, 4 * B), F32),
            pltpu.VMEM((4, 8, 4 * B), F32),
            pltpu.VMEM((4, 8, B), F32),
            pltpu.VMEM((4, 16, 8, B), F32),
            pltpu.VMEM((2, 16, B), F32),
            pltpu.VMEM((4, 8, 4 * B), F32),
            pltpu.VMEM((4, 8, 2 * B, 4 * B), BF16),
            pltpu.VMEM((4, 8, 2 * B, 4 * B), BF16),
            pltpu.VMEM((4, 2, B, 4 * B), F32),
            pltpu.VMEM((16, B, B), BF16),
            pltpu.VMEM((16, B, 2 * B), BF16),
            pltpu.VMEM((8, 2, B, B), F32),
            pltpu.VMEM((2, 2, B, B), F32),
            pltpu.VMEM((8, 2, B, B), BF16),
            pltpu.VMEM((8, 2, B, B), BF16),
            pltpu.VMEM((8, 2, B, B), BF16),
            pltpu.VMEM((7, 2, B, B), BF16),
            blocks, blocks,
            dma((2,)),
            dma((1,)), dma((26,)),
            dma((1,)), dma((4,)),
            dma((1,)), dma((8,)),
            dma((1,)), dma((8,)),
            dma((1,)), dma((1,)),
        ],
        compiler_params=pltpu.CompilerParams(
            collective_id=0, has_side_effects=True, vmem_limit_bytes=63 * 1024 * 1024
        ),
        name="attention_backward",
    )(queries, key_rows, value_rows, grad_output, positions.reshape(-1, B))
    return grads[0], grads[1], grads[2]


def solution(mesh):
    spec = P(("row", "col"), None)
    return jax.shard_map(
        body,
        mesh=mesh,
        in_specs=(spec, spec, spec, spec, P()),
        out_specs=(spec, spec, spec),
        check_vma=False,
    )
```

```python
import math

import jax
import jax.numpy as jnp
from jax import lax
from jax.experimental import pallas as pl
from jax.experimental.pallas import tpu as pltpu
from jax.sharding import PartitionSpec as P

MESH = pl.DeviceIdType.MESH
F32 = jnp.float32
BF16 = jnp.bfloat16
B = 128
NEG = -1e30
FLOOR = -1e6
LOG2E = math.log2(math.e)


def device(x, y, z, c):
    return (y * 2 + lax.rem(z, 2), (x * 4 + lax.div(z, 2)) * 2 + c)


def nt(a, b):
    return lax.dot_general(a, b, (((1,), (1,)), ((), ())), preferred_element_type=F32)


def nn(a, b):
    return jnp.dot(a, b, preferred_element_type=F32)


def kernel(
    q_ref, k_ref, v_ref, g_ref, pos_hbm, out_ref,
    qb, gb, kvb, pos_ref, ktb, posk, posq, s_buf, dp_buf, mt, zt, dt, stat_out, stat_in, factor, tops,
    w_buf, e_buf, sums, q_scaled, g_scaled, part, tmp, pair_out, pair_in, z_out, z_in, q_out, q_in,
    ins, gs, gr, ss, sr, ps, pr, zs, zr, qs_sem, qr_sem,
):
    row, col = lax.axis_index("row"), lax.axis_index("col")
    y, zlo = lax.div(row, 2), lax.rem(row, 2)
    x, c = lax.div(col, 8), lax.rem(col, 2)
    z = lax.rem(lax.div(col, 2), 4) * 2 + zlo
    up4 = lambda a, d: lax.rem(a + d, 4)
    up8 = lambda a, d: lax.rem(a + d, 8)
    other = 1 - c
    mine = x * 4 + y
    chip_scale = LOG2E / math.sqrt(B)

    here_k = z * 2 + c
    fetch = [
        pltpu.make_async_copy(src, dst, ins.at[n])
        for src, dst, n in (
            (
                (k_ref, kvb.at[here_k, 0], 0),
                (v_ref, kvb.at[here_k, 1], 0),
                (q_ref, qb.at[mine], 0),
                (g_ref, gb.at[mine], 0),
                (pos_hbm, pos_ref, 1),
            )
        )
    ]
    for copy in fetch:
        copy.start()

    plane = [lax.rem(mine + d, 16) for d in range(1, 16)]
    plane_dev = [device(lax.div(s, 4), lax.rem(s, 4), z, c) for s in plane]
    barrier = pltpu.get_barrier_semaphore()
    peers = [device(up4(x, d), y, z, c) for d in (2, 1, 3)] + [device(x, up4(y, d), z, c) for d in (2, 1, 3)]
    peers += [device(x, y, up8(z, d), c) for d in (2, 6, 1, 7)] + [device(x, y, z, other)]
    for p in peers:
        pl.semaphore_signal(barrier, inc=1, device_id=p, device_id_type=MESH)
    pltpu.make_async_copy(qb.at[0:4], qb.at[0:4], ins.at[0]).wait()
    pl.semaphore_wait(barrier, len(peers))

    to_pair = device(x, y, z, other)

    def whole(ref, send_sem, recv_sem):
        return pltpu.make_async_remote_copy(
            src_ref=ref, dst_ref=ref, send_sem=send_sem, recv_sem=recv_sem, device_id=to_pair, device_id_type=MESH
        )

    def send(src, to, n):
        pltpu.make_async_remote_copy(
            src_ref=src, dst_ref=src, send_sem=gs.at[0], recv_sem=gr.at[n], device_id=to, device_id_type=MESH
        ).start()

    done = set()

    def need(n, ref):
        if n not in done:
            done.add(n)
            whole(ref, gs.at[0], gr.at[n]).wait_recv()

    slot = lambda a, b: a * 4 + b
    xr, xl, yr, yl = up4(x, 1), up4(x, 3), up4(y, 1), up4(y, 3)
    x2, y2 = up4(x, 2), up4(y, 2)
    to_xr, to_xl = device(xr, y, z, c), device(xl, y, z, c)
    to_yr, to_yl = device(x, yr, z, c), device(x, yl, z, c)
    to_x2, to_y2 = device(x2, y, z, c), device(x, y2, z, c)
    plans = (
        (16, qb, lambda i, j: slot(i, j), x, y, (xl, xr, x2), (to_xr, to_xl, to_x2), (to_yr, to_yl, to_y2)),
        (19, gb, lambda i, j: slot(j, i), y, x, (yl, yr, y2), (to_yr, to_yl, to_y2), (to_xr, to_xl, to_x2)),
    )
    kv_at = lambda off: kvb.at[up8(z, off) * 2 + c]
    up = lambda d: device(x, y, up8(z, d), c)

    def send_across(p, n, src):
        to_b = plans[p][-1]
        for m in (2, 0, 1):
            send(src, to_b[m], 22 + (n if p == 0 else m))

    def send_pair(off):
        if off == 4:
            need(4, kv_at(4).at[0])
            need(0, kv_at(4).at[1])
        elif off:
            need(off, kv_at(off))
        send(kv_at(off), to_pair, 8 + off)

    def need_pair(*offs):
        for off in offs:
            need(8 + off, kv_at(off))

    send(kv_at(0), up(2), 6)
    send(kv_at(0), up(6), 2)
    for p, (first, buf, at, a, b, ias, to_a, to_b) in enumerate(plans):
        src = buf.at[at(a, b)]
        for n in (2, 0, 1):
            send(src, to_a[n], first + n)
        send_across(p, 3, src)
    send(kv_at(0), up(1), 7)
    send(kv_at(0), up(7), 1)
    send_pair(0)

    fetch[4].wait()
    zhi_col = lax.div(z, 2) * 2 + c
    for s in range(16):
        i, j = s // 4, s % 4
        posq[pl.ds(s, 1), :] = pos_ref[pl.ds((j * 2 + zlo) * 32 + i * 8 + zhi_col, 1), :].astype(F32)
    for s in range(16):
        zz, cc = s // 2, s % 2
        line = pos_ref[pl.ds((y * 2 + zz % 2) * 32 + (x * 4 + zz // 2) * 2 + cc, 1), :].astype(F32)
        posk[s] = jnp.broadcast_to(line, (B, B)).T

    def tile(t, zz):
        q_tile = qb[pl.ds(4 * t, 4)].reshape(4 * B, B)
        g_tile = gb[pl.ds(4 * t, 4)].reshape(4 * B, B)
        k_tile = kvb[pl.ds(2 * zz, 2), 0].reshape(2 * B, B)
        v_tile = kvb[pl.ds(2 * zz, 2), 1].reshape(2 * B, B)
        pq = jnp.concatenate([posq[pl.ds(4 * t + j, 1), :] for j in range(4)], axis=1)
        pk = posk[pl.ds(2 * zz, 2)].reshape(2 * B, B)
        pk = jnp.concatenate([pk] * 4, axis=1)
        s = jnp.where(pq >= pk, nt(k_tile, q_tile) * chip_scale, NEG)
        s_buf[t, zz] = s
        m = jnp.maximum(jnp.max(s, axis=0, keepdims=True), FLOOR)
        dp = nt(v_tile, g_tile)
        dp_buf[t, zz] = dp
        w = jnp.exp2(s - m)
        mt[t, pl.ds(zz, 1), :] = m
        zt[t, pl.ds(zz, 1), :] = jnp.sum(w, axis=0, keepdims=True)
        dt[t, pl.ds(zz, 1), :] = jnp.sum(w * dp, axis=0, keepdims=True)

    def tiles(n, pick):
        def step(i, carry):
            for t, zz in pick(i):
                tile(t, zz)
            return carry

        lax.fori_loop(0, n, step, 0)

    near = lambda i: up8(z, i + 5 * lax.div(i, 2))
    both = lambda i, d: up8(z, d + i * (8 - 2 * d))

    def across(n):
        for p, (first, buf, at, a, b, ias, to_a, to_b) in enumerate(plans):
            src = buf.at[at(ias[n], b)]
            need(first + n, src)
            send_across(p, n, src)

    across(0)
    across(1)
    need(6, kv_at(6))
    send(kv_at(6).at[0], up(2), 4)
    send(kv_at(6), up(1), 5)
    need(2, kv_at(2))
    send(kv_at(2).at[1], up(6), 0)
    send(kv_at(2), up(7), 3)
    across(2)
    for off in (1, 7, 2, 6):
        send_pair(off)

    def need_column(n):
        need(22 + n, qb.at[0 : 7 if n < 3 else 3])

    need_column(3)
    need_pair(0, 1, 7)
    tiles(3, lambda i: [(x, near(i))])
    need_pair(2, 6)
    tiles(1, lambda i: [(x, both(0, 2)), (x, both(1, 2))])
    need_column(0)
    need_column(1)
    tiles(3, lambda i: [(xl, near(i)), (xr, near(i))])
    for off in (3, 5, 4):
        send_pair(off)
    tiles(2, lambda i: [(xl, both(i, 2)), (xr, both(i, 2))])
    need_column(2)
    tiles(3, lambda i: [(x2, near(i))])
    tiles(1, lambda i: [(x2, both(0, 2)), (x2, both(1, 2))])
    need_pair(3, 5)
    tiles(4, lambda i: [(i, both(0, 3)), (i, both(1, 3))])
    need_pair(4)

    def finish(t, carry):
        tile(t, up8(z, 4))
        maxes = mt[t]
        top = jnp.max(maxes, axis=0, keepdims=True)
        tops[t, 0:1, :] = top
        f = jnp.exp2(maxes - top)
        total = jnp.sum(zt[t] * f, axis=0, keepdims=True)
        dot = jnp.sum(dt[t] * f, axis=0, keepdims=True)
        some = total > 0.0
        safe = jnp.where(some, total, 1.0)
        level = jnp.where(some, top + jnp.log(safe) * LOG2E, NEG)
        mean = dot / safe
        tops[t, 1:2, :] = mean
        for j in range(4):
            stat_out[t, pl.ds(j, 1), :] = level[:, j * B : (j + 1) * B]
            stat_out[t, pl.ds(4 + j, 1), :] = mean[:, j * B : (j + 1) * B]
        stat_in[t, mine] = stat_out[t]
        for d in range(15):
            pltpu.make_async_remote_copy(
                src_ref=stat_out.at[t], dst_ref=stat_in.at[t, mine], send_sem=ss.at[0], recv_sem=sr.at[t],
                device_id=plane_dev[d], device_id_type=MESH,
            ).start()
        return carry

    lax.fori_loop(0, 4, finish, 0)

    for zz in range(8):
        ktb[zz] = kvb[pl.ds(2 * zz, 2), 0].reshape(2 * B, B).T

    def weigh(t, carry):
        top, mean = tops[t, 0:1, :], tops[t, 1:2, :]
        of_e = of_w = None
        for zz in range(9):
            if zz < 8:
                w = jnp.exp2(s_buf[t, zz] - top)
                w_buf[t, zz] = w.astype(BF16)
                e_buf[t, zz] = (w * (dp_buf[t, zz] - mean)).astype(BF16)
            if zz:
                by_e, by_w = (nn(ktb[zz - 1], buf[t, zz - 1]) for buf in (e_buf, w_buf))
                of_e, of_w = (by_e, by_w) if zz == 1 else (of_e + by_e, of_w + by_w)
        sums[t, 0] = of_e
        sums[t, 1] = of_w
        return carry

    lax.fori_loop(0, 4, weigh, 0)

    def combine(t, carry):
        whole(stat_in.at[t, 0:15], ss.at[0], sr.at[t]).wait_recv()
        level = stat_in[t, :, 0:4, :]
        mean = stat_in[t, :, 4:8, :]
        top = jnp.max(level, axis=0)
        e = jnp.exp2(level - top[None])
        total = jnp.sum(e, axis=0)
        lse = top + jnp.log(total) * LOG2E
        delta = jnp.sum(e * mean, axis=0) / total
        for j in range(4):
            here = slice(j * B, (j + 1) * B)
            f = jnp.exp2(tops[t, 0:1, here] - lse[j : j + 1])
            h = (tops[t, 1:2, here] - delta[j : j + 1]) * f
            factor[0, pl.ds(4 * t + j, 1), :] = f
            factor[1, pl.ds(4 * t + j, 1), :] = h
        return carry

    lax.fori_loop(0, 4, combine, 0)

    column = lambda i: up4(x, (2, 1, 3, 0)[i])

    def q_copy(i, j):
        return pltpu.make_async_remote_copy(
            src_ref=q_out.at[4 * i + up4(y, j)], dst_ref=q_in.at[4 * i + j], send_sem=qs_sem.at[0], recv_sem=qr_sem.at[0],
            device_id=device(column(i), up4(y, j), z, c), device_id_type=MESH,
        )

    def query_side(i):
        t = column(i)
        for j in range(4):
            here = slice(j * B, (j + 1) * B)
            f = factor[0, pl.ds(4 * t + j, 1), :]
            h = factor[1, pl.ds(4 * t + j, 1), :]
            q_out[4 * i + j] = (sums[t, 0, :, here] * f + sums[t, 1, :, here] * h).astype(BF16)
        for j in (2, 1, 3, 0):
            if (i, j) != (3, 0):
                q_copy(i, j).start()

    f_col, h_col = factor[0].T, factor[1].T
    for s in range(16):
        f, h = f_col[:, s : s + 1], h_col[:, s : s + 1]
        rows = qb[s].astype(F32)
        q_scaled[s] = (rows * f).astype(BF16)
        g_scaled[s, :, :B] = (gb[s].astype(F32) * f).astype(BF16)
        g_scaled[s, :, B:] = (rows * h).astype(BF16)

    def pair_copy(off):
        return pltpu.make_async_remote_copy(
            src_ref=pair_out.at[off], dst_ref=pair_in.at[off], send_sem=ps.at[0], recv_sem=pr.at[off],
            device_id=to_pair, device_id_type=MESH,
        )

    to_z = lambda d: device(x, y, up8(z, d), c)

    def z_copy(n, src, dst, d):
        return pltpu.make_async_remote_copy(
            src_ref=src, dst_ref=dst, send_sem=zs.at[0], recv_sem=zr.at[n], device_id=to_z(d), device_id_type=MESH
        )

    hops = {
        4: (z_copy(0, z_out.at[4, 0], z_in.at[0, 0], 2), z_copy(1, z_out.at[4, 1], z_in.at[0, 1], 6)),
        3: (z_copy(2, z_out.at[3], z_in.at[1], 1),),
        5: (z_copy(3, z_out.at[5], z_in.at[2], 7),),
        2: (z_copy(4, z_out.at[2], z_in.at[3], 2),),
        6: (z_copy(5, z_out.at[6], z_in.at[4], 6),),
        1: (z_copy(6, z_out.at[1], z_in.at[5], 1),),
        7: (z_copy(7, z_out.at[7], z_in.at[6], 7),),
    }

    def pass_on(off):
        pair_copy(off).wait_recv()
        for w in range(2):
            total = part[off, w] + pair_in[off, w].astype(F32)
            if off in (2, 6):
                if w == 0:
                    hops[3 if off == 2 else 5][0].wait_recv()
                total += z_in[1 if off == 2 else 2, w].astype(F32)
                if w == (0 if off == 2 else 1):
                    hops[4][w].wait_recv()
                    total += z_in[0, w].astype(F32)
            z_out[off, w] = total.astype(BF16)
        for copy in hops[off]:
            copy.start()

    def key_side(off):
        zz = up8(z, off)
        e_row, w_row = (jnp.concatenate([buf[t, zz] for t in range(4)], axis=1) for buf in (e_buf, w_buf))
        dk = nn(e_row, q_scaled[...].reshape(16 * B, B))
        dvk = nn(w_row, g_scaled[...].reshape(16 * B, 2 * B))
        for w, total in enumerate((dk + dvk[:, B:], dvk[:, :B])):
            tmp[w] = total.reshape(2, B, B)
            part[off, w] = tmp[w, c]
            pair_out[off, w] = tmp[w, other].astype(BF16)
        pair_copy(off).start()

    key_side(4)
    key_side(3)
    query_side(0)
    key_side(5)
    pass_on(4)
    query_side(1)
    query_side(2)
    query_side(3)
    key_side(1)
    pass_on(3)
    key_side(7)
    pass_on(5)
    key_side(2)
    pass_on(1)
    key_side(6)
    pass_on(7)
    key_side(0)
    pass_on(2)
    pass_on(6)

    scale = 1.0 / math.sqrt(B)
    pair_copy(0).wait_recv()
    acc = [part[0, w] + pair_in[0, w].astype(F32) for w in range(2)]
    own = q_out[12 + y].astype(F32)
    whole(q_in.at[0:15], qs_sem.at[0], qr_sem.at[0]).wait_recv()
    for n in range(16):
        if n != 12:
            own += q_in[n].astype(F32)
    out_ref[0] = (own * scale).T.astype(BF16)
    for off, n in ((1, 5), (7, 6), (2, 3), (6, 4)):
        hops[off][0].wait_recv()
        for w in range(2):
            acc[w] += z_in[n, w].astype(F32)
    out_ref[1] = (acc[0] * scale).astype(BF16)
    out_ref[2] = acc[1].astype(BF16)

    whole(s_buf.at[0, 0:5, 0:192, :], gs.at[0], gr.at[0]).wait_send()
    whole(stat_in.at[:, 0:15], ss.at[0], sr.at[0]).wait_send()
    whole(pair_out, ps.at[0], pr.at[0]).wait_send()
    whole(z_out.at[1:8], zs.at[0], zr.at[0]).wait_send()
    whole(q_in.at[0:15], qs_sem.at[0], qr_sem.at[0]).wait_send()


def body(queries, key_rows, value_rows, grad_output, positions):
    vmem = pl.BlockSpec(memory_space=pltpu.VMEM)
    hbm = pl.BlockSpec(memory_space=pl.ANY)
    dma = pltpu.SemaphoreType.DMA
    blocks = pltpu.VMEM((16, B, B), BF16)
    grads = pl.pallas_call(
        kernel,
        out_shape=jax.ShapeDtypeStruct((3, B, B), BF16),
        in_specs=[hbm] * 5,
        out_specs=vmem,
        scratch_shapes=[
            blocks, blocks,
            pltpu.VMEM((16, 2, B, B), BF16),
            pltpu.VMEM((256, B), jnp.int32),
            pltpu.VMEM((8, B, 2 * B), BF16),
            pltpu.VMEM((16, B, B), F32),
            pltpu.VMEM((16, B), F32),
            pltpu.VMEM((4, 8, 2 * B, 4 * B), F32),
            pltpu.VMEM((4, 8, 2 * B, 4 * B), F32),
            pltpu.VMEM((4, 8, 4 * B), F32),
            pltpu.VMEM((4, 8, 4 * B), F32),
            pltpu.VMEM((4, 8, 4 * B), F32),
            pltpu.VMEM((4, 8, B), F32),
            pltpu.VMEM((4, 16, 8, B), F32),
            pltpu.VMEM((2, 16, B), F32),
            pltpu.VMEM((4, 8, 4 * B), F32),
            pltpu.VMEM((4, 8, 2 * B, 4 * B), BF16),
            pltpu.VMEM((4, 8, 2 * B, 4 * B), BF16),
            pltpu.VMEM((4, 2, B, 4 * B), F32),
            pltpu.VMEM((16, B, B), BF16),
            pltpu.VMEM((16, B, 2 * B), BF16),
            pltpu.VMEM((8, 2, B, B), F32),
            pltpu.VMEM((2, 2, B, B), F32),
            pltpu.VMEM((8, 2, B, B), BF16),
            pltpu.VMEM((8, 2, B, B), BF16),
            pltpu.VMEM((8, 2, B, B), BF16),
            pltpu.VMEM((7, 2, B, B), BF16),
            blocks, blocks,
            dma((2,)),
            dma((1,)), dma((26,)),
            dma((1,)), dma((4,)),
            dma((1,)), dma((8,)),
            dma((1,)), dma((8,)),
            dma((1,)), dma((1,)),
        ],
        compiler_params=pltpu.CompilerParams(
            collective_id=0, has_side_effects=True, vmem_limit_bytes=63 * 1024 * 1024
        ),
        name="attention_backward",
    )(queries, key_rows, value_rows, grad_output, positions.reshape(-1, B))
    return grads[0], grads[1], grads[2]


def solution(mesh):
    spec = P(("row", "col"), None)
    return jax.shard_map(
        body,
        mesh=mesh,
        in_specs=(spec, spec, spec, spec, P()),
        out_specs=(spec, spec, spec),
        check_vma=False,
    )
```
